32 devices in a mesh: dp: 2 (over x), cp: 4 (over z), tp: 4 (over y, core).
Axes of the slice: x: 2, y: 2, z: 4, core: 2. Of those that a mesh axis runs over, the one named last changes fastest.
Arguments:
- x_tok: bfloat16 [16384, 1024], P(('dp', 'cp', 'tp')), parts along dimension 0
- w_q: bfloat16 [1024, 32, 32], P(None, 'tp')
- w_k: bfloat16 [1024, 8, 32], P(None, 'tp')
- w_v: bfloat16 [1024, 8, 32], P(None, 'tp')
- w_o: bfloat16 [32, 32, 1024], P('tp')
- expert_ids: int32 [16384, 2], P(('dp', 'cp', 'tp')), parts along dimension 0
- gate_wts: float32 [16384, 2], P(('dp', 'cp', 'tp')), parts along dimension 0
- w_gate: bfloat16 [16, 1024, 1792], P(('cp', 'tp'))
- w_up: bfloat16 [16, 1024, 1792], P(('cp', 'tp'))
- w_down: bfloat16 [16, 1792, 1024], P(('cp', 'tp'))
Outputs:
- output: bfloat16 [16384, 1024], P(('dp', 'cp', 'tp')), parts along dimension 0
There are 2 independent parts. The reference program is written for one: setup_inputs(seed, part) draws one part's arguments, and reference() takes and returns one part's arrays. A program takes and returns all parts, laid end to end along the dimension named above; an argument that names none is the same for every part.
All inputs are finite; a program needn't handle non-finite values.
Results may differ from the reference program's by a relative error of at most 0.0113248.
Values are sent between devices in bfloat16 or wider.
A program may use at most 1 GiB of HBM per device.

```python
import math
import jax
import jax.numpy as jnp
from jax import lax

TOK_DEV = 512
CP = 4
TP = 4
HID = 1024
FFN = 3584
HEADS = 32
KV_HEADS = 8
HEAD = 32
EXPERTS = 8
TOP = 2

SEQ = TOK_DEV * CP * TP
BLOCKS = CP * TP
PAIRS = CP * TP // 2
LOCAL = EXPERTS // PAIRS
HALF_FFN = FFN // 2
GROUP = HEADS // KV_HEADS


def token_positions():
    half_len = SEQ // CP
    chunk_len = half_len // 2
    row_ids = jnp.arange(SEQ)
    cp_rank = row_ids // half_len
    in_half = row_ids % half_len
    return jnp.where(in_half < chunk_len, cp_rank * chunk_len + in_half, (2 * CP - 1 - cp_rank) * chunk_len + in_half - chunk_len)


def draw_routing(route_key):
    perm_key, label_key = jax.random.split(route_key)
    tok_order = jax.vmap(lambda one_key: jax.random.permutation(one_key, TOK_DEV))(jax.random.split(perm_key, BLOCKS))
    relabel = jax.vmap(lambda one_key: jax.random.permutation(one_key, EXPERTS))(jax.random.split(label_key, BLOCKS))
    raw_ids = (tok_order[:, :, None] + jnp.arange(TOP)[None, None, :]) % EXPERTS
    picked = jax.vmap(lambda label_map, raw_set: label_map[raw_set])(relabel, raw_ids)
    return picked.reshape(SEQ, TOP).astype(jnp.int32)


def setup_inputs(seed: int = 0, part: int = 0) -> dict:
    part_key = jax.random.fold_in(jax.random.key(seed), part)
    key_x, key_route, key_gate = jax.random.split(part_key, 3)
    weight_keys = jax.random.split(jax.random.key(seed + 1), 7)
    score_gain = math.sqrt(max(math.log(SEQ / 8.0), 1.0))
    in_scale = 1.0 / math.sqrt(HID)
    x_tok = jax.random.normal(key_x, (SEQ, HID), jnp.float32).astype(jnp.bfloat16)
    w_q = (jax.random.normal(weight_keys[0], (HID, HEADS, HEAD), jnp.float32) * (score_gain * in_scale)).astype(jnp.bfloat16)
    w_k = (jax.random.normal(weight_keys[1], (HID, KV_HEADS, HEAD), jnp.float32) * in_scale).astype(jnp.bfloat16)
    w_v = (jax.random.normal(weight_keys[2], (HID, KV_HEADS, HEAD), jnp.float32) * in_scale).astype(jnp.bfloat16)
    w_o = (jax.random.normal(weight_keys[3], (HEADS, HEAD, HID), jnp.float32) * (2.0 / math.sqrt(HEADS * HEAD))).astype(jnp.bfloat16)
    w_gate = (jax.random.normal(weight_keys[4], (2 * EXPERTS, HID, HALF_FFN), jnp.float32) * in_scale).astype(jnp.bfloat16)
    w_up = (jax.random.normal(weight_keys[5], (2 * EXPERTS, HID, HALF_FFN), jnp.float32) * in_scale).astype(jnp.bfloat16)
    w_down = (jax.random.normal(weight_keys[6], (2 * EXPERTS, HALF_FFN, HID), jnp.float32) * (2.0 / math.sqrt(FFN))).astype(jnp.bfloat16)
    gate_raw = jax.random.uniform(key_gate, (SEQ, TOP), jnp.float32, 1.0, 3.0)
    gate_wts = gate_raw / jnp.sum(gate_raw, axis=1, keepdims=True)
    expert_ids = draw_routing(key_route)
    return {"x_tok": x_tok, "w_q": w_q, "w_k": w_k, "w_v": w_v, "w_o": w_o, "expert_ids": expert_ids, "gate_wts": gate_wts, "w_gate": w_gate, "w_up": w_up, "w_down": w_down}


def reference(x_tok, w_q, w_k, w_v, w_o, expert_ids, gate_wts, w_gate, w_up, w_down):
    q_all = jnp.dot(x_tok, w_q.reshape(HID, HEADS * HEAD), preferred_element_type=jnp.float32).astype(jnp.bfloat16)
    k_all = jnp.dot(x_tok, w_k.reshape(HID, KV_HEADS * HEAD), preferred_element_type=jnp.float32).astype(jnp.bfloat16)
    v_all = jnp.dot(x_tok, w_v.reshape(HID, KV_HEADS * HEAD), preferred_element_type=jnp.float32).astype(jnp.bfloat16)
    q_blocks = q_all.reshape(BLOCKS, TOK_DEV, KV_HEADS, GROUP, HEAD)
    positions = token_positions()
    pos_blocks = positions.reshape(BLOCKS, TOK_DEV)
    keys_f = k_all.reshape(SEQ, KV_HEADS, HEAD).astype(jnp.float32)
    vals_f = v_all.reshape(SEQ, KV_HEADS, HEAD).astype(jnp.float32)
    score_scale = HEAD ** -0.5

    def attend(blk_item):
        q_blk, q_pos = blk_item
        scores = jnp.einsum("qgrd,kgd->grqk", q_blk.astype(jnp.float32), keys_f) * score_scale
        allowed = q_pos[:, None] >= positions[None, :]
        scores = jnp.where(allowed[None, None], scores, -jnp.inf)
        row_peak = jnp.max(scores, axis=-1, keepdims=True)
        prob_vals = jnp.exp(scores - row_peak)
        row_sum = jnp.sum(prob_vals, axis=-1)
        mixed_vals = jnp.einsum("grqk,kgd->qgrd", prob_vals.astype(jnp.bfloat16).astype(jnp.float32), vals_f)
        return (mixed_vals / jnp.moveaxis(row_sum, -1, 0)[..., None]).astype(jnp.bfloat16)

    attn_out = lax.map(attend, (q_blocks, pos_blocks)).reshape(SEQ, HEADS * HEAD)
    h_tok = (x_tok.astype(jnp.float32) + jnp.dot(attn_out, w_o.reshape(HEADS * HEAD, HID), preferred_element_type=jnp.float32)).astype(jnp.bfloat16)

    full_gate = w_gate.reshape(PAIRS, 2, LOCAL, HID, HALF_FFN).transpose(0, 2, 3, 1, 4).reshape(EXPERTS, HID, FFN)
    full_up = w_up.reshape(PAIRS, 2, LOCAL, HID, HALF_FFN).transpose(0, 2, 3, 1, 4).reshape(EXPERTS, HID, FFN)
    full_down = w_down.reshape(PAIRS, 2, LOCAL, HALF_FFN, HID).transpose(0, 2, 1, 3, 4).reshape(EXPERTS, FFN, HID)
    flat_ids = expert_ids.reshape(-1)
    sort_order = jnp.argsort(flat_ids, stable=True)
    per_expert = SEQ * TOP // EXPERTS
    tok_rows = (sort_order // TOP).reshape(EXPERTS, per_expert)

    def run_expert(expert_item):
        rows_e, gate_e, up_e, down_e = expert_item
        tokens = h_tok[rows_e]
        gate_pre = jnp.dot(tokens, gate_e, preferred_element_type=jnp.float32)
        up_pre = jnp.dot(tokens, up_e, preferred_element_type=jnp.float32)
        hidden = (jax.nn.silu(gate_pre) * up_pre).astype(jnp.bfloat16)
        return jnp.dot(hidden, down_e, preferred_element_type=jnp.float32).astype(jnp.bfloat16)

    z_sorted = lax.map(run_expert, (tok_rows, full_gate, full_up, full_down)).reshape(SEQ * TOP, HID)
    back_order = jnp.argsort(sort_order)
    z_choice = z_sorted[back_order].reshape(SEQ, TOP, HID)
    y_acc = h_tok.astype(jnp.float32)
    for choice in range(TOP):
        y_acc = y_acc + gate_wts[:, choice:choice + 1] * z_choice[:, choice].astype(jnp.float32)
    return y_acc.astype(jnp.bfloat16)
```

```python
import functools
import math

import jax
import jax.numpy as jnp
from jax import lax
from jax.experimental import pallas as pl
from jax.experimental.pallas import tpu as pltpu
from jax.sharding import PartitionSpec as P


def attn_kernel(n_cp, chunk, bq, bk, heads, grp, q_ref, k_ref, v_ref, o_ref, m_ref, l_ref, acc_ref):
    head_dim = acc_ref.shape[1]
    cp_index = lax.axis_index("cp")
    step = pl.program_id(0)
    q_per = chunk // bq
    k_per = chunk // bk
    half = step // q_per
    in_chunk = step % q_per
    my_chunk = jnp.where(half == 0, cp_index, 2 * n_cp - 1 - cp_index)
    diag = (in_chunk * bq) // bk
    score_scale = head_dim ** -0.5 * math.log2(math.e)

    def key_offset(blk):
        chunk_id = blk // k_per
        rank = jnp.where(chunk_id < n_cp, chunk_id, 2 * n_cp - 1 - chunk_id)
        upper = jnp.where(chunk_id < n_cp, 0, 1)
        return rank * (2 * chunk) + upper * chunk + (blk % k_per) * bk

    def visit(blk, first):
        off = pl.multiple_of(key_offset(blk), bk)
        k_blk = k_ref[pl.ds(off, bk), :]
        v_blk = v_ref[:, pl.ds(off, bk)]
        if first:
            k_pos = diag * bk + lax.broadcasted_iota(jnp.int32, (bk, bq), 0)
            q_pos = in_chunk * bq + lax.broadcasted_iota(jnp.int32, (bk, bq), 1)
            allowed = k_pos <= q_pos
        for head in range(heads):
            kv = head // grp
            scores = jnp.dot(k_blk, q_ref[head], preferred_element_type=jnp.float32)
            if first:
                scores = jnp.where(allowed, scores, -1e30)
            top = jnp.max(scores, axis=0, keepdims=True)
            if not first:
                old = m_ref[head]
                top = jnp.maximum(old, top)
            prob = jnp.exp2((scores - top) * score_scale)
            part = jnp.sum(prob.reshape(bk // 8, 8, bq), axis=0)
            mixed = jnp.dot(v_blk[kv * head_dim:(kv + 1) * head_dim], prob.astype(jnp.bfloat16), preferred_element_type=jnp.float32)
            m_ref[head] = top
            if first:
                l_ref[head] = part
                acc_ref[head] = mixed
            else:
                rescale = jnp.exp2((old - top) * score_scale)
                l_ref[head] = l_ref[head] * rescale + part
                acc_ref[head] = acc_ref[head] * rescale + mixed

    base = my_chunk * k_per
    visit(base + diag, True)

    def body(blk, carry):
        visit(blk, False)
        return carry

    lax.fori_loop(0, base + diag, body, 0)
    for head in range(heads):
        total = jnp.sum(l_ref[head], axis=0, keepdims=True)
        o_ref[head] = (acc_ref[head] / total).astype(o_ref.dtype)


def attention(q_t, k_all, v_all, n_cp, head_dim, bq=256, bk=512):
    heads, depth, rows = q_t.shape
    chunk = rows // 2
    n_keys = k_all.shape[0]
    grp = heads // (depth // head_dim)
    pairs = heads * rows * n_keys // 2
    return pl.pallas_call(
        functools.partial(attn_kernel, n_cp, chunk, bq, bk, heads, grp),
        out_shape=jax.ShapeDtypeStruct((heads, head_dim, rows), jnp.bfloat16),
        grid=(rows // bq,),
        in_specs=[
            pl.BlockSpec((heads, depth, bq), lambda i: (0, 0, i)),
            pl.BlockSpec((n_keys, depth), lambda i: (0, 0)),
            pl.BlockSpec((depth, n_keys), lambda i: (0, 0)),
        ],
        out_specs=pl.BlockSpec((heads, head_dim, bq), lambda i: (0, 0, i)),
        scratch_shapes=[
            pltpu.VMEM((heads, 1, bq), jnp.float32),
            pltpu.VMEM((heads, 8, bq), jnp.float32),
            pltpu.VMEM((heads, head_dim, bq), jnp.float32),
        ],
        compiler_params=pltpu.CompilerParams(dimension_semantics=("arbitrary",), vmem_limit_bytes=48 * 1024 * 1024),
        cost_estimate=pl.CostEstimate(flops=4 * pairs * 64, bytes_accessed=8 * 1024 * 1024, transcendentals=pairs),
        name="causal_attention",
    )(q_t, k_all, v_all)


def solution(mesh):
    n_cp = mesh.shape["cp"]
    n_tp = mesh.shape["tp"]
    row_spec = P(("dp", "cp", "tp"), None)
    head_spec = P(None, "tp", None)
    expert_spec = P(("cp", "tp"), None, None)

    def device_step(x_loc, w_q, w_k, w_v, w_o, ids_loc, gates_loc, w_gate, w_up, w_down):
        tok_dev, hid_dim = x_loc.shape
        top_k = ids_loc.shape[1]
        kv_loc = w_k.shape[1]
        heads = w_q.shape[1]
        head_dim = w_q.shape[2]
        grp_size = heads // kv_loc
        local_exp = w_gate.shape[0]
        n_experts = local_exp * n_cp * n_tp // 2
        capacity = top_k * tok_dev // n_experts
        half_hid = hid_dim // 2
        tp_index = lax.axis_index("tp")
        n_slots = n_experts * capacity

        choice_hot = (ids_loc[:, :, None] == jnp.arange(n_experts)[None, None, :])
        token_hot = jnp.sum(choice_hot.astype(jnp.bfloat16), axis=1)
        earlier = (lax.broadcasted_iota(jnp.int32, (tok_dev, tok_dev), 0) > lax.broadcasted_iota(jnp.int32, (tok_dev, tok_dev), 1)).astype(jnp.bfloat16)
        rank_in = jnp.dot(earlier, token_hot, preferred_element_type=jnp.float32).astype(jnp.int32)
        place = rank_in + jnp.arange(n_experts, dtype=jnp.int32)[None, :] * capacity
        dest_idx = jnp.sum(jnp.where(choice_hot, place[:, None, :], 0), axis=2)

        x_half = lax.all_gather(x_loc, "tp", axis=0, tiled=True)
        half_len = x_half.shape[0]
        q_t = jnp.einsum("sh,hnd->nds", x_half, w_q, preferred_element_type=jnp.float32).astype(jnp.bfloat16)
        q_t = q_t.reshape(kv_loc, grp_size, head_dim, half_len)
        q_t = jnp.concatenate([jnp.pad(q_t[kv], ((0, 0), (kv * head_dim, (kv_loc - 1 - kv) * head_dim), (0, 0))) for kv in range(kv_loc)], axis=0)
        k_cur = jnp.einsum("sh,hnd->snd", x_half, w_k, preferred_element_type=jnp.float32).astype(jnp.bfloat16).reshape(half_len, kv_loc * head_dim)
        v_cur = jnp.einsum("sh,hnd->nds", x_half, w_v, preferred_element_type=jnp.float32).astype(jnp.bfloat16).reshape(kv_loc * head_dim, half_len)
        k_all = lax.all_gather(k_cur, "cp", axis=0, tiled=True)
        v_all = lax.all_gather(v_cur, "cp", axis=1, tiled=True)
        out_t = attention(q_t, k_all, v_all, n_cp, head_dim)
        out_t = out_t.reshape(heads * head_dim, n_tp, tok_dev)
        out_t = lax.all_to_all(out_t, "tp", 1, 0, tiled=True).reshape(n_tp * heads * head_dim, tok_dev)
        w_o_all = lax.all_gather(w_o.reshape(heads * head_dim, hid_dim), "tp", axis=0, tiled=True)
        attn_rows = lax.dot_general(out_t, w_o_all, (((0,), (0,)), ((), ())), preferred_element_type=jnp.float32)
        h_loc = (x_loc.astype(jnp.float32) + attn_rows).astype(jnp.bfloat16)

        slots = jnp.arange(n_slots, dtype=jnp.int32)
        pick = (slots[:, None] == dest_idx[:, 0][None, :]) | (slots[:, None] == dest_idx[:, 1][None, :])
        send_buf = jnp.dot(pick.astype(jnp.bfloat16), h_loc, preferred_element_type=jnp.float32).astype(jnp.bfloat16)
        send_buf = send_buf.reshape(n_cp, n_tp // 2, 1, local_exp, capacity, hid_dim)
        send_buf = jnp.broadcast_to(send_buf, (n_cp, n_tp // 2, 2, local_exp, capacity, hid_dim)).reshape(n_cp, n_tp, local_exp, capacity, hid_dim)
        recv_buf = lax.all_to_all(send_buf, "tp", 1, 1, tiled=True)
        recv_buf = lax.all_to_all(recv_buf, "cp", 0, 0, tiled=True)

        gate_pre = jnp.einsum("uvech,ehf->uvecf", recv_buf, w_gate, preferred_element_type=jnp.float32)
        up_pre = jnp.einsum("uvech,ehf->uvecf", recv_buf, w_up, preferred_element_type=jnp.float32)
        hidden = (jax.nn.silu(gate_pre) * up_pre).astype(jnp.bfloat16)
        z_part = jnp.einsum("uvecf,efh->uvech", hidden, w_down, preferred_element_type=jnp.float32)

        my_half = tp_index % 2
        keep_part = lax.dynamic_slice_in_dim(z_part, my_half * half_hid, half_hid, axis=4)
        send_part = lax.dynamic_slice_in_dim(z_part, (1 - my_half) * half_hid, half_hid, axis=4)
        pair_perm = [(dev_idx, dev_idx ^ 1) for dev_idx in range(n_tp)]
        z_half = (keep_part + lax.ppermute(send_part, "tp", pair_perm)).astype(jnp.bfloat16)

        back_buf = lax.all_to_all(z_half, "cp", 0, 0, tiled=True)
        back_buf = lax.all_to_all(back_buf, "tp", 1, 1, tiled=True)
        z_full = back_buf.reshape(n_cp, n_tp // 2, 2, local_exp, capacity, half_hid).transpose(0, 1, 3, 4, 2, 5).reshape(n_slots, hid_dim)
        y_loc = h_loc.astype(jnp.float32)
        for choice in range(top_k):
            take = (dest_idx[:, choice][:, None] == slots[None, :]).astype(jnp.bfloat16)
            y_loc = y_loc + gates_loc[:, choice:choice + 1] * jnp.dot(take, z_full, preferred_element_type=jnp.float32)
        return y_loc.astype(jnp.bfloat16)

    return jax.shard_map(device_step, mesh=mesh, in_specs=(row_spec, head_spec, head_spec, head_spec, P("tp", None, None), row_spec, row_spec, expert_spec, expert_spec, expert_spec), out_specs=row_spec, check_vma=False)
```

```python
import functools
import math

import jax
import jax.numpy as jnp
from jax import lax
from jax.experimental import pallas as pl
from jax.experimental.pallas import tpu as pltpu
from jax.sharding import PartitionSpec as P


def attn_kernel(n_cp, chunk, bq, bk, heads, grp, q_ref, k_ref, v_ref, o_ref, m_ref, l_ref, acc_ref):
    head_dim = acc_ref.shape[1]
    cp_index = lax.axis_index("cp")
    step = pl.program_id(0)
    q_per = chunk // bq
    k_per = chunk // bk
    half = step // q_per
    in_chunk = step % q_per
    my_chunk = jnp.where(half == 0, cp_index, 2 * n_cp - 1 - cp_index)
    diag = (in_chunk * bq) // bk
    score_scale = head_dim ** -0.5 * math.log2(math.e)

    def key_offset(blk):
        chunk_id = blk // k_per
        rank = jnp.where(chunk_id < n_cp, chunk_id, 2 * n_cp - 1 - chunk_id)
        upper = jnp.where(chunk_id < n_cp, 0, 1)
        return rank * (2 * chunk) + upper * chunk + (blk % k_per) * bk

    def visit(blk, first):
        off = pl.multiple_of(key_offset(blk), bk)
        k_blk = k_ref[pl.ds(off, bk), :]
        v_blk = v_ref[:, pl.ds(off, bk)]
        if first:
            k_pos = diag * bk + lax.broadcasted_iota(jnp.int32, (bk, bq), 0)
            q_pos = in_chunk * bq + lax.broadcasted_iota(jnp.int32, (bk, bq), 1)
            allowed = k_pos <= q_pos
        for head in range(heads):
            kv = head // grp
            scores = jnp.dot(k_blk, q_ref[head], preferred_element_type=jnp.float32)
            if first:
                scores = jnp.where(allowed, scores, -1e30)
            top = jnp.max(scores, axis=0, keepdims=True)
            if not first:
                old = m_ref[head]
                top = jnp.maximum(old, top)
            prob = jnp.exp2((scores - top) * score_scale)
            part = jnp.sum(prob.reshape(bk // 8, 8, bq), axis=0)
            mixed = jnp.dot(v_blk[kv * head_dim:(kv + 1) * head_dim], prob.astype(jnp.bfloat16), preferred_element_type=jnp.float32)
            m_ref[head] = top
            if first:
                l_ref[head] = part
                acc_ref[head] = mixed
            else:
                rescale = jnp.exp2((old - top) * score_scale)
                l_ref[head] = l_ref[head] * rescale + part
                acc_ref[head] = acc_ref[head] * rescale + mixed

    base = my_chunk * k_per
    visit(base + diag, True)

    def body(blk, carry):
        visit(blk, False)
        return carry

    lax.fori_loop(0, base + diag, body, 0)
    for head in range(heads):
        total = jnp.sum(l_ref[head], axis=0, keepdims=True)
        o_ref[head] = (acc_ref[head] / total).astype(o_ref.dtype)


def attention(q_t, k_all, v_all, n_cp, head_dim, bq=256, bk=512):
    heads, depth, rows = q_t.shape
    chunk = rows // 2
    n_keys = k_all.shape[0]
    grp = heads // (depth // head_dim)
    pairs = heads * rows * n_keys // 2
    return pl.pallas_call(
        functools.partial(attn_kernel, n_cp, chunk, bq, bk, heads, grp),
        out_shape=jax.ShapeDtypeStruct((heads, head_dim, rows), jnp.bfloat16),
        grid=(rows // bq,),
        in_specs=[
            pl.BlockSpec((heads, depth, bq), lambda i: (0, 0, i)),
            pl.BlockSpec((n_keys, depth), lambda i: (0, 0)),
            pl.BlockSpec((depth, n_keys), lambda i: (0, 0)),
        ],
        out_specs=pl.BlockSpec((heads, head_dim, bq), lambda i: (0, 0, i)),
        scratch_shapes=[
            pltpu.VMEM((heads, 1, bq), jnp.float32),
            pltpu.VMEM((heads, 8, bq), jnp.float32),
            pltpu.VMEM((heads, head_dim, bq), jnp.float32),
        ],
        compiler_params=pltpu.CompilerParams(dimension_semantics=("arbitrary",), vmem_limit_bytes=48 * 1024 * 1024),
        cost_estimate=pl.CostEstimate(flops=4 * pairs * 64, bytes_accessed=8 * 1024 * 1024, transcendentals=pairs),
        name="causal_attention",
    )(q_t, k_all, v_all)


MESH_ID = pl.DeviceIdType.MESH


def flip_bits(index, pattern, n_bits):
    result = 0
    for bit in range(n_bits):
        digit = (index // (1 << bit)) % 2
        result = result + ((1 - digit) if (pattern >> bit) & 1 else digit) * (1 << bit)
    return result


def expert_kernel(n_chips, order, rounds, h_ref, gate_a, gate_b, up_a, up_b, down_a, down_b, z_ref,
                  recv, w_gate, w_up, w_down, act, total, z_out, load_sem, own_sem, send_sem, recv_sem, back_sem, home_sem):
    n_bits = n_chips.bit_length() - 1
    dp_index = lax.axis_index("dp")
    cp_index = lax.axis_index("cp")
    tp_index = lax.axis_index("tp")
    core = tp_index % 2
    chip = cp_index * 2 + tp_index // 2

    def peer(pattern):
        other = flip_bits(chip, pattern, n_bits)
        return (dp_index, other // 2, (other % 2) * 2 + core)

    loads = []
    for half, refs in enumerate(((gate_a, up_a, down_a), (gate_b, up_b, down_b))):
        for which, (src, dst) in enumerate(zip(refs, (w_gate, w_up, w_down))):
            loads.append(pltpu.make_async_copy(src.at[0], dst.at[half], load_sem.at[half, which]))
    for load in loads:
        load.start()
    own = pltpu.make_async_copy(h_ref.at[0], recv.at[0], own_sem.at[0])
    own.start()

    barrier = pltpu.get_barrier_semaphore()
    for pattern in range(1, n_chips):
        pl.semaphore_signal(barrier, inc=1, device_id=peer(pattern), device_id_type=MESH_ID)
    pl.semaphore_wait(barrier, n_chips - 1)

    sends = {}
    for pattern in order:
        sends[pattern] = pltpu.make_async_remote_copy(
            src_ref=h_ref.at[pattern], dst_ref=recv.at[pattern], send_sem=send_sem.at[pattern], recv_sem=recv_sem.at[pattern],
            device_id=peer(pattern), device_id_type=MESH_ID)
        sends[pattern].start()

    rows = recv.shape[1]
    hid = recv.shape[2]
    ffn = w_gate.shape[2]
    tile = 256
    backs = {}
    own.wait()
    for turn, (first, second) in enumerate(rounds):
        for pattern in (first, second):
            if pattern:
                sends[pattern].wait_recv()
        for half in range(2):
            if turn == 0:
                loads[half * 3].wait()
                loads[half * 3 + 1].wait()

        x_blk = jnp.concatenate([recv[first], recv[second]], axis=0)

        def half_step(half, carry):
            for col in range(0, ffn, tile):
                gate_pre = jnp.dot(x_blk, w_gate[half, :, col:col + tile], preferred_element_type=jnp.float32)
                up_pre = jnp.dot(x_blk, w_up[half, :, col:col + tile], preferred_element_type=jnp.float32)
                act[half, :, col:col + tile] = (jax.nn.silu(gate_pre) * up_pre).astype(jnp.bfloat16)
            return carry

        lax.fori_loop(0, 2, half_step, 0)
        if turn == 0:
            for half in range(2):
                loads[half * 3 + 2].wait()

        def out_step(col, carry):
            at = pl.multiple_of(col * tile, tile)
            z_blk = jnp.dot(act[0], w_down[0, :, pl.ds(at, tile)], preferred_element_type=jnp.float32)
            z_blk = z_blk + jnp.dot(act[1], w_down[1, :, pl.ds(at, tile)], preferred_element_type=jnp.float32)
            z_blk = z_blk.astype(jnp.bfloat16)
            z_out[first, :, pl.ds(at, tile)] = z_blk[:rows]
            z_out[second, :, pl.ds(at, tile)] = z_blk[rows:]
            return carry

        lax.fori_loop(0, hid // tile, out_step, 0)
        for pattern in (first, second):
            if pattern:
                backs[pattern] = pltpu.make_async_remote_copy(
                    src_ref=z_out.at[pattern], dst_ref=z_ref.at[pattern], send_sem=back_sem.at[pattern], recv_sem=home_sem.at[pattern],
                    device_id=peer(pattern), device_id_type=MESH_ID)
            else:
                backs[pattern] = pltpu.make_async_copy(z_out.at[pattern], z_ref.at[pattern], own_sem.at[1])
            backs[pattern].start()
    for pattern in order:
        sends[pattern].wait_send()
    for pattern in range(n_chips):
        backs[pattern].wait()


def expert_layer(send_buf, own_weights, other_weights):
    n_chips, rows, hid = send_buf.shape
    ffn = own_weights[0].shape[2]
    order = (1, 4, 6, 5, 7, 2, 3)
    rounds = ((0, 1), (4, 6), (5, 7), (2, 3))
    weights = []
    for own, other in zip(own_weights, other_weights):
        weights += [own, other]
    any_spec = pl.BlockSpec(memory_space=pl.ANY)
    flops = 2 * 3 * n_chips * rows * hid * 2 * ffn
    return pl.pallas_call(
        functools.partial(expert_kernel, n_chips, order, rounds),
        out_shape=jax.ShapeDtypeStruct((n_chips, rows, hid), jnp.bfloat16),
        in_specs=[any_spec] * 7,
        out_specs=any_spec,
        scratch_shapes=[
            pltpu.VMEM((n_chips, rows, hid), jnp.bfloat16),
            pltpu.VMEM((2, hid, ffn), jnp.bfloat16),
            pltpu.VMEM((2, hid, ffn), jnp.bfloat16),
            pltpu.VMEM((2, ffn, hid), jnp.bfloat16),
            pltpu.VMEM((2, 2 * rows, ffn), jnp.bfloat16),
            pltpu.VMEM((8, 128), jnp.float32),
            pltpu.VMEM((n_chips, rows, hid), jnp.bfloat16),
            pltpu.SemaphoreType.DMA((2, 3)),
            pltpu.SemaphoreType.DMA((2,)),
            pltpu.SemaphoreType.DMA((n_chips,)),
            pltpu.SemaphoreType.DMA((n_chips,)),
            pltpu.SemaphoreType.DMA((n_chips,)),
            pltpu.SemaphoreType.DMA((n_chips,)),
        ],
        compiler_params=pltpu.CompilerParams(collective_id=1, has_side_effects=True, vmem_limit_bytes=58 * 1024 * 1024),
        cost_estimate=pl.CostEstimate(flops=flops, bytes_accessed=32 * 1024 * 1024, transcendentals=n_chips * rows * 2 * ffn),
        name="expert_layer",
    )(send_buf, *weights)


def solution(mesh):
    n_cp = mesh.shape["cp"]
    n_tp = mesh.shape["tp"]
    row_spec = P(("dp", "cp", "tp"), None)
    head_spec = P(None, "tp", None)
    expert_spec = P(("cp", "tp"), None, None)

    def device_step(x_loc, w_q, w_k, w_v, w_o, ids_loc, gates_loc, w_gate, w_up, w_down):
        tok_dev, hid_dim = x_loc.shape
        top_k = ids_loc.shape[1]
        kv_loc = w_k.shape[1]
        heads = w_q.shape[1]
        head_dim = w_q.shape[2]
        grp_size = heads // kv_loc
        local_exp = w_gate.shape[0]
        n_experts = local_exp * n_cp * n_tp // 2
        capacity = top_k * tok_dev // n_experts
        chip = lax.axis_index("cp") * 2 + lax.axis_index("tp") // 2
        n_slots = n_experts * capacity

        pair_perm = [(dev_idx, dev_idx ^ 1) for dev_idx in range(n_tp)]
        other_weights = [lax.ppermute(one, "tp", pair_perm) for one in (w_gate, w_up, w_down)]

        choice_hot = (ids_loc[:, :, None] == jnp.arange(n_experts)[None, None, :])
        token_hot = jnp.sum(choice_hot.astype(jnp.bfloat16), axis=1)
        earlier = (lax.broadcasted_iota(jnp.int32, (tok_dev, tok_dev), 0) > lax.broadcasted_iota(jnp.int32, (tok_dev, tok_dev), 1)).astype(jnp.bfloat16)
        rank_in = jnp.dot(earlier, token_hot, preferred_element_type=jnp.float32).astype(jnp.int32)
        place = rank_in + (jnp.arange(n_experts, dtype=jnp.int32) ^ chip)[None, :] * capacity
        dest_idx = jnp.sum(jnp.where(choice_hot, place[:, None, :], 0), axis=2)

        x_half = lax.all_gather(x_loc, "tp", axis=0, tiled=True)
        half_len = x_half.shape[0]
        q_t = jnp.einsum("sh,hnd->nds", x_half, w_q, preferred_element_type=jnp.float32).astype(jnp.bfloat16)
        q_t = q_t.reshape(kv_loc, grp_size, head_dim, half_len)
        q_t = jnp.concatenate([jnp.pad(q_t[kv], ((0, 0), (kv * head_dim, (kv_loc - 1 - kv) * head_dim), (0, 0))) for kv in range(kv_loc)], axis=0)
        k_cur = jnp.einsum("sh,hnd->snd", x_half, w_k, preferred_element_type=jnp.float32).astype(jnp.bfloat16).reshape(half_len, kv_loc * head_dim)
        v_cur = jnp.einsum("sh,hnd->nds", x_half, w_v, preferred_element_type=jnp.float32).astype(jnp.bfloat16).reshape(kv_loc * head_dim, half_len)
        k_all = lax.all_gather(k_cur, "cp", axis=0, tiled=True)
        v_all = lax.all_gather(v_cur, "cp", axis=1, tiled=True)
        out_t = attention(q_t, k_all, v_all, n_cp, head_dim)
        out_t = out_t.reshape(heads * head_dim, n_tp, tok_dev)
        out_t = lax.all_to_all(out_t, "tp", 1, 0, tiled=True).reshape(n_tp * heads * head_dim, tok_dev)
        w_o_all = lax.all_gather(w_o.reshape(heads * head_dim, hid_dim), "tp", axis=0, tiled=True)
        attn_rows = lax.dot_general(out_t, w_o_all, (((0,), (0,)), ((), ())), preferred_element_type=jnp.float32)
        h_loc = (x_loc.astype(jnp.float32) + attn_rows).astype(jnp.bfloat16)

        slots = jnp.arange(n_slots, dtype=jnp.int32)
        pick = (slots[:, None] == dest_idx[:, 0][None, :]) | (slots[:, None] == dest_idx[:, 1][None, :])
        send_buf = jnp.dot(pick.astype(jnp.bfloat16), h_loc, preferred_element_type=jnp.float32).astype(jnp.bfloat16)
        z_full = expert_layer(send_buf.reshape(n_experts, capacity, hid_dim), (w_gate, w_up, w_down), other_weights).reshape(n_slots, hid_dim)
        y_loc = h_loc.astype(jnp.float32)
        for choice in range(top_k):
            take = (dest_idx[:, choice][:, None] == slots[None, :]).astype(jnp.bfloat16)
            y_loc = y_loc + gates_loc[:, choice:choice + 1] * jnp.dot(take, z_full, preferred_element_type=jnp.float32)
        return y_loc.astype(jnp.bfloat16)

    return jax.shard_map(device_step, mesh=mesh, in_specs=(row_spec, head_spec, head_spec, head_spec, P("tp", None, None), row_spec, row_spec, expert_spec, expert_spec, expert_spec), out_specs=row_spec, check_vma=False)
```

```python
import functools
import math

import jax
import jax.numpy as jnp
from jax import lax
from jax.experimental import pallas as pl
from jax.experimental.pallas import tpu as pltpu
from jax.sharding import PartitionSpec as P


MESH_ID = pl.DeviceIdType.MESH


def project_kernel(pieces, x_ref, w_q_ref, w_k_ref, w_v_ref, q_ref, k_ref, v_ref, x_all, k_dup, pair_send, pair_recv, far_send, far_recv, pass_send, pass_recv):
    dp_index = lax.axis_index("dp")
    cp_index = lax.axis_index("cp")
    me = lax.axis_index("tp")
    pair = me + 1 - 2 * (me % 2)
    far = (me + 2) % 4
    far_pair = (pair + 2) % 4
    tok = x_ref.shape[0]
    rows = tok // pieces

    barrier = pltpu.get_barrier_semaphore()
    for other in (pair, far):
        pl.semaphore_signal(barrier, inc=1, device_id=(dp_index, cp_index, other), device_id_type=MESH_ID)
    pl.semaphore_wait(barrier, 2)

    def piece(ref, num):
        return ref.at[pl.ds(num * rows, rows)]

    far_copies, pass_copies = [], []
    for num in range(pieces):
        far_copies.append(pltpu.make_async_remote_copy(
            src_ref=piece(x_ref, num), dst_ref=x_all.at[me, pl.ds(num * rows, rows)], send_sem=far_send.at[num], recv_sem=far_recv.at[num],
            device_id=(dp_index, cp_index, far), device_id_type=MESH_ID))
        far_copies[num].start()
        pass_copies.append(pltpu.make_async_remote_copy(
            src_ref=x_all.at[far, pl.ds(num * rows, rows)], dst_ref=x_all.at[far, pl.ds(num * rows, rows)], send_sem=pass_send.at[num], recv_sem=pass_recv.at[num],
            device_id=(dp_index, cp_index, pair), device_id_type=MESH_ID))
    pair_copy = pltpu.make_async_remote_copy(
        src_ref=x_ref, dst_ref=x_all.at[me], send_sem=pair_send.at[0], recv_sem=pair_recv.at[0],
        device_id=(dp_index, cp_index, pair), device_id_type=MESH_ID)
    pair_copy.start()

    contract = (((1,), (1,)), ((), ()))

    def project(x_blk, block, start, size):
        q_ref[block, :, start:start + size] = lax.dot_general(w_q_ref[...], x_blk, contract, preferred_element_type=jnp.float32).astype(jnp.bfloat16)
        v_ref[block, :, start:start + size] = lax.dot_general(w_v_ref[...], x_blk, contract, preferred_element_type=jnp.float32).astype(jnp.bfloat16)
        w_k = w_k_ref[...]
        k_blk = lax.dot_general(x_blk, jnp.concatenate([w_k, w_k], axis=0), contract, preferred_element_type=jnp.float32)
        k_dup[block, start:start + size, :] = k_blk.astype(jnp.bfloat16)

    project(x_ref[...], me, 0, tok)
    pair_copy.wait_recv()
    project(x_all[pair], pair, 0, tok)
    for num in range(pieces):
        far_copies[num].wait_recv()
        pass_copies[num].start()
        project(x_all[far, num * rows:(num + 1) * rows], far, num * rows, rows)
        pass_copies[num].wait_recv()
        project(x_all[far_pair, num * rows:(num + 1) * rows], far_pair, num * rows, rows)
    low = lax.broadcasted_iota(jnp.int32, k_dup.shape[1:], 1) < k_dup.shape[2] // 2
    for half in range(2):
        k_ref[half] = jnp.where(low, k_dup[2 * half].astype(jnp.float32), k_dup[2 * half + 1].astype(jnp.float32)).astype(jnp.bfloat16)
    pair_copy.wait_send()
    for num in range(pieces):
        far_copies[num].wait_send()
        pass_copies[num].wait_send()


def project_rows(x_loc, w_q, w_k, w_v, n_tp):
    tok, hid = x_loc.shape
    pieces = 4
    depth_q = w_q.shape[0]
    depth_k = w_k.shape[0]
    vmem = pl.BlockSpec(memory_space=pltpu.VMEM)
    return pl.pallas_call(
        functools.partial(project_kernel, pieces),
        out_shape=(
            jax.ShapeDtypeStruct((n_tp, depth_q, tok), jnp.bfloat16),
            jax.ShapeDtypeStruct((n_tp // 2, tok, 2 * depth_k), jnp.bfloat16),
            jax.ShapeDtypeStruct((n_tp, depth_k, tok), jnp.bfloat16),
        ),
        in_specs=[vmem] * 4,
        out_specs=(vmem, vmem, vmem),
        scratch_shapes=[
            pltpu.VMEM((n_tp, tok, hid), jnp.bfloat16),
            pltpu.VMEM((n_tp, tok, 2 * depth_k), jnp.bfloat16),
            pltpu.SemaphoreType.DMA((1,)),
            pltpu.SemaphoreType.DMA((1,)),
            pltpu.SemaphoreType.DMA((pieces,)),
            pltpu.SemaphoreType.DMA((pieces,)),
            pltpu.SemaphoreType.DMA((pieces,)),
            pltpu.SemaphoreType.DMA((pieces,)),
        ],
        compiler_params=pltpu.CompilerParams(collective_id=0, has_side_effects=True, vmem_limit_bytes=40 * 1024 * 1024),
        cost_estimate=pl.CostEstimate(flops=2 * n_tp * tok * hid * (depth_q + 2 * depth_k), bytes_accessed=8 * 1024 * 1024, transcendentals=0),
        name="project_rows",
    )(x_loc, w_q, w_k, w_v)


def attn_kernel(n_cp, n_tp, heads, grp, head_dim, q_ref, kc_ref, vc_ref, w_o_ref, gate_ref, up_ref, down_ref,
                o_ref, w_o_all, gate_other, up_other, down_other,
                q3_ref, kc_all, v_all, k_exp, m_ref, old_ref, l_ref, acc_ref, s0_ref, s1_ref, o_send,
                k_send, k_recv, v_send, v_recv, local_sem, wo_send, wo_recv, ex_send, ex_recv, out_send, out_recv):
    dp_index = lax.axis_index("dp")
    me = lax.axis_index("cp")
    tp_index = lax.axis_index("tp")
    blk = q_ref.shape[2]
    kv_heads = heads // grp
    depth = k_exp.shape[2] // kv_heads
    score_scale = head_dim ** -0.5 * math.log2(math.e)
    s_refs = (s0_ref, s1_ref)
    near = me + 1 - 2 * (me % 2)
    mid = 2 - me // 2
    end = 3 * (1 - me // 2)
    others = (near, mid, end)

    def cp_peer(rank):
        return (dp_index, rank, tp_index)

    def tp_peer(rank):
        return (dp_index, me, rank)

    barrier = pltpu.get_barrier_semaphore()
    for rank in others:
        pl.semaphore_signal(barrier, inc=1, device_id=cp_peer(rank), device_id_type=MESH_ID)
    for shift in range(1, n_tp):
        pl.semaphore_signal(barrier, inc=1, device_id=tp_peer((tp_index + shift) % n_tp), device_id_type=MESH_ID)
    pl.semaphore_wait(barrier, n_cp - 1 + n_tp - 1)

    def key_copies(step, half, rank, owner):
        k_copy = pltpu.make_async_remote_copy(
            src_ref=kc_ref.at[half], dst_ref=kc_all.at[owner * 2 + half], send_sem=k_send.at[step, half], recv_sem=k_recv.at[owner, half],
            device_id=cp_peer(rank), device_id_type=MESH_ID)
        v_copy = pltpu.make_async_remote_copy(
            src_ref=vc_ref.at[pl.ds(half * 2, 2)], dst_ref=v_all.at[pl.ds((owner * 2 + half) * 2, 2)], send_sem=v_send.at[step, half], recv_sem=v_recv.at[owner, half],
            device_id=cp_peer(rank), device_id_type=MESH_ID)
        return k_copy, v_copy

    for step, rank in enumerate(others):
        for copy in key_copies(step, 0, rank, me):
            copy.start()

        @pl.when(rank < me)
        def _():
            for copy in key_copies(step, 1, rank, me):
                copy.start()

    wo_copies = [pltpu.make_async_copy(w_o_ref, w_o_all.at[0], local_sem.at[0])]
    for shift in range(1, n_tp):
        wo_copies.append(pltpu.make_async_remote_copy(
            src_ref=w_o_ref, dst_ref=w_o_all.at[shift], send_sem=wo_send.at[shift], recv_sem=wo_recv.at[shift],
            device_id=tp_peer((tp_index + shift) % n_tp), device_id_type=MESH_ID))
    pair = tp_index + 1 - 2 * (tp_index % 2)
    ex_copies = []
    for which, (src, dst) in enumerate(((gate_ref, gate_other), (up_ref, up_other), (down_ref, down_other))):
        ex_copies.append(pltpu.make_async_remote_copy(
            src_ref=src, dst_ref=dst, send_sem=ex_send.at[which], recv_sem=ex_recv.at[which], device_id=tp_peer(pair), device_id_type=MESH_ID))
    for copy in wo_copies + ex_copies:
        copy.start()

    for block in range(n_tp):
        for head in range(heads):
            rest = q_ref[block, head * head_dim:(head + 1) * head_dim, :].astype(jnp.float32) * score_scale
            for term in range(3):
                part = rest.astype(jnp.bfloat16)
                q3_ref[block, head, term * head_dim:(term + 1) * head_dim, :] = part
                rest = rest - part.astype(jnp.float32)
            q3_ref[block, head, 3 * head_dim:, :] = jnp.zeros((depth - 3 * head_dim, blk), jnp.bfloat16)
    m_ref[...] = jnp.full(m_ref.shape, -1e30, jnp.float32)
    l_ref[...] = jnp.zeros(l_ref.shape, jnp.float32)
    acc_ref[...] = jnp.zeros(acc_ref.shape, jnp.float32)

    lane = lax.broadcasted_iota(jnp.int32, (kc_ref.shape[2], k_exp.shape[2]), 0)
    col = lax.broadcasted_iota(jnp.int32, (kc_ref.shape[2], k_exp.shape[2]), 1)
    spread = [(lane == sub * (kv_heads * head_dim) + (col // depth) * head_dim + col % head_dim).astype(jnp.bfloat16) for sub in range(2)]

    def expand(k_half, at):
        for sub in range(2):
            k_exp[at * 2 + sub] = jnp.dot(k_half, spread[sub], preferred_element_type=jnp.float32).astype(jnp.bfloat16)

    def score(head, block, at, masked):
        kv = head // grp
        scores = jnp.dot(k_exp[at, :, kv * depth:(kv + 1) * depth], q3_ref[block, head], preferred_element_type=jnp.float32)
        if masked:
            k_pos = lax.broadcasted_iota(jnp.int32, (blk, blk), 0)
            q_pos = lax.broadcasted_iota(jnp.int32, (blk, blk), 1)
            scores = jnp.where(k_pos <= q_pos, scores, -1e30)
        s_refs[head % 2][...] = scores
        old = m_ref[block, head]
        old_ref[head] = old
        m_ref[block, head] = jnp.maximum(old, jnp.max(scores, axis=0, keepdims=True))

    def mix(head, block, at):
        kv = head // grp
        top = m_ref[block, head]
        prob = jnp.exp2(s_refs[head % 2][...] - top)
        part = jnp.sum(prob.reshape(blk // 8, 8, blk), axis=0)
        mixed = jnp.dot(v_all[at, kv * head_dim:(kv + 1) * head_dim, :], prob.astype(jnp.bfloat16), preferred_element_type=jnp.float32)
        rescale = jnp.exp2(old_ref[head] - top)
        l_ref[block, head] = l_ref[block, head] * rescale + part
        acc_ref[block, head] = acc_ref[block, head] * rescale + mixed

    def run(count, place, masked):
        block, at = place(0)
        score(0, block, at, masked)

        def body(num, carry):
            block, at = place(num)
            next_block, next_at = place(num + 1 - (num + 1) // count)
            for head in range(heads):
                if head + 1 < heads:
                    score(head + 1, block, at, masked)
                else:
                    score(0, next_block, next_at, masked)
                mix(head, block, at)
            return carry

        lax.fori_loop(0, count, body, 0)

    for half in range(2):
        expand(kc_ref[half], me * 2 + half)
        for sub in range(2):
            v_all[(me * 2 + half) * 2 + sub] = vc_ref[half * 2 + sub]

    def place_diag(num):
        return num, me * 4 + num

    def place_local(num):
        late = (num + 2) // 4
        block = (1 - late) * (1 + 2 * num) + late * (1 + num // 2)
        half = (1 - late) * num
        return block, me * 4 + half * 2 + late * (num % 2)

    run(4, place_diag, True)
    run(6, place_local, False)

    def visit_rank(step, carry):
        rank = ((2 - step) // 2) * near + (step % 2) * mid + (step // 2) * end
        below = (me - rank + 3) // 4
        for copy in key_copies(0, 0, rank, rank):
            copy.wait_recv()
        expand(kc_all[rank * 2], rank * 2)

        @pl.when(rank > me)
        def _():
            for copy in key_copies(0, 1, rank, rank):
                copy.wait_recv()
            expand(kc_all[rank * 2 + 1], rank * 2 + 1)

        def place(num):
            block = below * (num // 2) + (1 - below) * (2 + num // 4)
            half = (1 - below) * ((num // 2) % 2)
            return block, rank * 4 + half * 2 + num % 2

        run(8, place, False)
        return carry

    lax.fori_loop(0, n_cp - 1, visit_rank, 0)

    outs = []
    for shift in (2, 1, 3, 0):
        block = (tp_index + shift) % n_tp
        for head in range(heads):
            total = jnp.sum(l_ref[block, head], axis=0, keepdims=True)
            o_send[block, head * head_dim:(head + 1) * head_dim, :] = (acc_ref[block, head] / total).astype(jnp.bfloat16)
        if shift:
            outs.append(pltpu.make_async_remote_copy(
                src_ref=o_send.at[block], dst_ref=o_ref.at[shift], send_sem=out_send.at[shift], recv_sem=out_recv.at[shift],
                device_id=tp_peer(block), device_id_type=MESH_ID))
        else:
            outs.append(pltpu.make_async_copy(o_send.at[block], o_ref.at[0], local_sem.at[1]))
        outs[-1].start()
    for step, rank in enumerate(others):
        for copy in key_copies(step, 0, rank, me):
            copy.wait_send()

        @pl.when(rank < me)
        def _():
            for copy in key_copies(step, 1, rank, me):
                copy.wait_send()

    for copy in wo_copies + ex_copies + outs:
        copy.wait()


def attention(q_t, k_c, v_c, w_o, experts, n_cp, head_dim, kv_heads):
    n_tp, q_depth, blk = q_t.shape
    heads = q_depth // head_dim
    grp = heads // kv_heads
    hid = w_o.shape[1]
    depth = 128
    pairs = heads * (n_tp * blk) ** 2 * n_cp // 2
    vmem = pl.BlockSpec(memory_space=pltpu.VMEM)
    any_spec = pl.BlockSpec(memory_space=pl.ANY)
    dma = pltpu.SemaphoreType.DMA
    return pl.pallas_call(
        functools.partial(attn_kernel, n_cp, n_tp, heads, grp, head_dim),
        out_shape=(
            jax.ShapeDtypeStruct((n_tp, q_depth, blk), jnp.bfloat16),
            jax.ShapeDtypeStruct((n_tp, q_depth, hid), jnp.bfloat16),
        ) + tuple(jax.ShapeDtypeStruct(one.shape, one.dtype) for one in experts),
        in_specs=[vmem] * 3 + [any_spec] * 4,
        out_specs=(any_spec,) * 5,
        scratch_shapes=[
            pltpu.VMEM((n_tp, heads, depth, blk), jnp.bfloat16),
            pltpu.VMEM((2 * n_cp,) + k_c.shape[1:], jnp.bfloat16),
            pltpu.VMEM((4 * n_cp,) + v_c.shape[1:], jnp.bfloat16),
            pltpu.VMEM((4 * n_cp, blk, kv_heads * depth), jnp.bfloat16),
            pltpu.VMEM((n_tp, heads, 1, blk), jnp.float32),
            pltpu.VMEM((heads, 1, blk), jnp.float32),
            pltpu.VMEM((n_tp, heads, 8, blk), jnp.float32),
            pltpu.VMEM((n_tp, heads, head_dim, blk), jnp.float32),
            pltpu.VMEM((blk, blk), jnp.float32),
            pltpu.VMEM((blk, blk), jnp.float32),
            pltpu.VMEM((n_tp, q_depth, blk), jnp.bfloat16),
            dma((n_cp - 1, 2)), dma((n_cp, 2)), dma((n_cp - 1, 2)), dma((n_cp, 2)), dma((2,)),
            dma((n_tp,)), dma((n_tp,)), dma((3,)), dma((3,)), dma((n_tp,)), dma((n_tp,)),
        ],
        compiler_params=pltpu.CompilerParams(collective_id=2, has_side_effects=True, vmem_limit_bytes=48 * 1024 * 1024),
        cost_estimate=pl.CostEstimate(flops=4 * pairs * 64, bytes_accessed=40 * 1024 * 1024, transcendentals=pairs),
        name="causal_attention",
    )(q_t, k_c, v_c, w_o, *experts)


def flip_bits(index, pattern, n_bits):
    result = 0
    for bit in range(n_bits):
        digit = (index // (1 << bit)) % 2
        result = result + ((1 - digit) if (pattern >> bit) & 1 else digit) * (1 << bit)
    return result


def expert_kernel(n_chips, order, rounds, h_ref, gate_a, gate_b, up_a, up_b, down_a, down_b, z_ref,
                  recv, w_gate, w_up, w_down, act, total, z_out, load_sem, own_sem, send_sem, recv_sem, back_sem, home_sem):
    n_bits = n_chips.bit_length() - 1
    dp_index = lax.axis_index("dp")
    cp_index = lax.axis_index("cp")
    tp_index = lax.axis_index("tp")
    core = tp_index % 2
    chip = cp_index * 2 + tp_index // 2

    def peer(pattern):
        other = flip_bits(chip, pattern, n_bits)
        return (dp_index, other // 2, (other % 2) * 2 + core)

    loads = []
    for half, refs in enumerate(((gate_a, up_a, down_a), (gate_b, up_b, down_b))):
        for which, (src, dst) in enumerate(zip(refs, (w_gate, w_up, w_down))):
            loads.append(pltpu.make_async_copy(src.at[0], dst.at[half], load_sem.at[half, which]))
    for load in loads:
        load.start()
    own = pltpu.make_async_copy(h_ref.at[0], recv.at[0], own_sem.at[0])
    own.start()

    barrier = pltpu.get_barrier_semaphore()
    for pattern in range(1, n_chips):
        pl.semaphore_signal(barrier, inc=1, device_id=peer(pattern), device_id_type=MESH_ID)
    pl.semaphore_wait(barrier, n_chips - 1)

    sends = {}
    for pattern in order:
        sends[pattern] = pltpu.make_async_remote_copy(
            src_ref=h_ref.at[pattern], dst_ref=recv.at[pattern], send_sem=send_sem.at[pattern], recv_sem=recv_sem.at[pattern],
            device_id=peer(pattern), device_id_type=MESH_ID)
        sends[pattern].start()

    rows = recv.shape[1]
    hid = recv.shape[2]
    ffn = w_gate.shape[2]
    tile = 256
    backs = {}
    own.wait()
    for turn, (first, second) in enumerate(rounds):
        for pattern in (first, second):
            if pattern:
                sends[pattern].wait_recv()
        for half in range(2):
            if turn == 0:
                loads[half * 3].wait()
                loads[half * 3 + 1].wait()

        x_blk = jnp.concatenate([recv[first], recv[second]], axis=0)

        def half_step(half, carry):
            for col in range(0, ffn, tile):
                gate_pre = jnp.dot(x_blk, w_gate[half, :, col:col + tile], preferred_element_type=jnp.float32)
                up_pre = jnp.dot(x_blk, w_up[half, :, col:col + tile], preferred_element_type=jnp.float32)
                act[half, :, col:col + tile] = (jax.nn.silu(gate_pre) * up_pre).astype(jnp.bfloat16)
            return carry

        lax.fori_loop(0, 2, half_step, 0)
        if turn == 0:
            for half in range(2):
                loads[half * 3 + 2].wait()

        def out_step(col, carry):
            at = pl.multiple_of(col * tile, tile)
            z_blk = jnp.dot(act[0], w_down[0, :, pl.ds(at, tile)], preferred_element_type=jnp.float32)
            z_blk = z_blk + jnp.dot(act[1], w_down[1, :, pl.ds(at, tile)], preferred_element_type=jnp.float32)
            z_blk = z_blk.astype(jnp.bfloat16)
            z_out[first, :, pl.ds(at, tile)] = z_blk[:rows]
            z_out[second, :, pl.ds(at, tile)] = z_blk[rows:]
            return carry

        lax.fori_loop(0, hid // tile, out_step, 0)
        for pattern in (first, second):
            if pattern:
                backs[pattern] = pltpu.make_async_remote_copy(
                    src_ref=z_out.at[pattern], dst_ref=z_ref.at[pattern], send_sem=back_sem.at[pattern], recv_sem=home_sem.at[pattern],
                    device_id=peer(pattern), device_id_type=MESH_ID)
            else:
                backs[pattern] = pltpu.make_async_copy(z_out.at[pattern], z_ref.at[pattern], own_sem.at[1])
            backs[pattern].start()
    for pattern in order:
        sends[pattern].wait_send()
    for pattern in range(n_chips):
        backs[pattern].wait()


def expert_layer(send_buf, own_weights, other_weights):
    n_chips, rows, hid = send_buf.shape
    ffn = own_weights[0].shape[2]
    order = (1, 4, 6, 5, 7, 2, 3)
    rounds = ((0, 1), (4, 6), (5, 7), (2, 3))
    weights = []
    for own, other in zip(own_weights, other_weights):
        weights += [own, other]
    any_spec = pl.BlockSpec(memory_space=pl.ANY)
    flops = 2 * 3 * n_chips * rows * hid * 2 * ffn
    return pl.pallas_call(
        functools.partial(expert_kernel, n_chips, order, rounds),
        out_shape=jax.ShapeDtypeStruct((n_chips, rows, hid), jnp.bfloat16),
        in_specs=[any_spec] * 7,
        out_specs=any_spec,
        scratch_shapes=[
            pltpu.VMEM((n_chips, rows, hid), jnp.bfloat16),
            pltpu.VMEM((2, hid, ffn), jnp.bfloat16),
            pltpu.VMEM((2, hid, ffn), jnp.bfloat16),
            pltpu.VMEM((2, ffn, hid), jnp.bfloat16),
            pltpu.VMEM((2, 2 * rows, ffn), jnp.bfloat16),
            pltpu.VMEM((8, 128), jnp.float32),
            pltpu.VMEM((n_chips, rows, hid), jnp.bfloat16),
            pltpu.SemaphoreType.DMA((2, 3)),
            pltpu.SemaphoreType.DMA((2,)),
            pltpu.SemaphoreType.DMA((n_chips,)),
            pltpu.SemaphoreType.DMA((n_chips,)),
            pltpu.SemaphoreType.DMA((n_chips,)),
            pltpu.SemaphoreType.DMA((n_chips,)),
        ],
        compiler_params=pltpu.CompilerParams(collective_id=1, has_side_effects=True, vmem_limit_bytes=58 * 1024 * 1024),
        cost_estimate=pl.CostEstimate(flops=flops, bytes_accessed=32 * 1024 * 1024, transcendentals=n_chips * rows * 2 * ffn),
        name="expert_layer",
    )(send_buf, *weights)


def solution(mesh):
    n_cp = mesh.shape["cp"]
    n_tp = mesh.shape["tp"]
    row_spec = P(("dp", "cp", "tp"), None)
    head_spec = P(None, "tp", None)
    expert_spec = P(("cp", "tp"), None, None)

    def device_step(x_loc, w_q, w_k, w_v, w_o, ids_loc, gates_loc, w_gate, w_up, w_down):
        tok_dev, hid_dim = x_loc.shape
        top_k = ids_loc.shape[1]
        kv_loc = w_k.shape[1]
        heads = w_q.shape[1]
        head_dim = w_q.shape[2]
        local_exp = w_gate.shape[0]
        n_experts = local_exp * n_cp * n_tp // 2
        capacity = top_k * tok_dev // n_experts
        chip = lax.axis_index("cp") * 2 + lax.axis_index("tp") // 2
        n_slots = n_experts * capacity

        choice_hot = (ids_loc[:, :, None] == jnp.arange(n_experts)[None, None, :])
        token_hot = jnp.sum(choice_hot.astype(jnp.bfloat16), axis=1)
        earlier = (lax.broadcasted_iota(jnp.int32, (tok_dev, tok_dev), 0) > lax.broadcasted_iota(jnp.int32, (tok_dev, tok_dev), 1)).astype(jnp.bfloat16)
        rank_in = jnp.dot(earlier, token_hot, preferred_element_type=jnp.float32).astype(jnp.int32)
        place = rank_in + (jnp.arange(n_experts, dtype=jnp.int32) ^ chip)[None, :] * capacity
        dest_idx = jnp.sum(jnp.where(choice_hot, place[:, None, :], 0), axis=2)

        q_t, k_c, v_c = project_rows(x_loc, *(one.transpose(1, 2, 0).reshape(-1, hid_dim) for one in (w_q, w_k, w_v)), n_tp)
        out_t, w_o_all, *other_weights = attention(q_t, k_c, v_c, w_o.reshape(heads * head_dim, hid_dim), (w_gate, w_up, w_down), n_cp, head_dim, kv_loc)
        out_t = out_t.reshape(n_tp * heads * head_dim, tok_dev)
        w_o_all = w_o_all.reshape(n_tp * heads * head_dim, hid_dim)
        attn_rows = lax.dot_general(out_t, w_o_all, (((0,), (0,)), ((), ())), preferred_element_type=jnp.float32)
        h_loc = (x_loc.astype(jnp.float32) + attn_rows).astype(jnp.bfloat16)

        slots = jnp.arange(n_slots, dtype=jnp.int32)
        pick = (slots[:, None] == dest_idx[:, 0][None, :]) | (slots[:, None] == dest_idx[:, 1][None, :])
        send_buf = jnp.dot(pick.astype(jnp.bfloat16), h_loc, preferred_element_type=jnp.float32).astype(jnp.bfloat16)
        z_full = expert_layer(send_buf.reshape(n_experts, capacity, hid_dim), (w_gate, w_up, w_down), other_weights).reshape(n_slots, hid_dim)
        y_loc = h_loc.astype(jnp.float32)
        for choice in range(top_k):
            take = (dest_idx[:, choice][:, None] == slots[None, :]).astype(jnp.bfloat16)
            y_loc = y_loc + gates_loc[:, choice:choice + 1] * jnp.dot(take, z_full, preferred_element_type=jnp.float32)
        return y_loc.astype(jnp.bfloat16)

    return jax.shard_map(device_step, mesh=mesh, in_specs=(row_spec, head_spec, head_spec, head_spec, P("tp", None, None), row_spec, row_spec, expert_spec, expert_spec, expert_spec), out_specs=row_spec, check_vma=False)
```

```python
import functools
import math

import jax
import jax.numpy as jnp
from jax import lax
from jax.experimental import pallas as pl
from jax.experimental.pallas import tpu as pltpu
from jax.sharding import PartitionSpec as P


MESH_ID = pl.DeviceIdType.MESH


def attn_kernel(n_cp, n_tp, heads, grp, head_dim, pieces, x_ref, w_q_ref, w_k_ref, w_v_ref, w_o_ref, gate_ref, up_ref, down_ref,
                o_ref, w_o_all, gate_other, up_other, down_other,
                x_all, w_q, w_k, w_v, k_dup, k_own, q3_ref, kc_all, v_all, k_exp, m_ref, old_ref, l_ref, acc_ref, s0_ref, s1_ref, o_send,
                load_sem, pair_sem, far_send, far_recv, pass_send, pass_recv,
                k_send, k_recv, v_send, v_recv, local_sem, wo_send, wo_recv, ex_send, ex_recv, out_send, out_recv):
    dp_index = lax.axis_index("dp")
    me = lax.axis_index("cp")
    tp_index = lax.axis_index("tp")
    blk = x_ref.shape[0]
    kv_heads = heads // grp
    depth = k_exp.shape[2] // kv_heads
    score_scale = head_dim ** -0.5 * math.log2(math.e)
    s_refs = (s0_ref, s1_ref)
    near = me + 1 - 2 * (me % 2)
    mid = 2 - me // 2
    end = 3 * (1 - me // 2)
    others = (near, mid, end)
    pair = tp_index + 1 - 2 * (tp_index % 2)
    far = (tp_index + 2) % 4
    far_pair = (pair + 2) % 4
    my_half = tp_index // 2
    rows = blk // pieces

    loads = [pltpu.make_async_copy(x_ref, x_all.at[tp_index], load_sem.at[0])]
    for num, (src, dst) in enumerate(((w_q_ref, w_q), (w_k_ref, w_k), (w_v_ref, w_v))):
        loads.append(pltpu.make_async_copy(src, dst, load_sem.at[num + 1]))
    for load in loads:
        load.start()

    def cp_peer(rank):
        return (dp_index, rank, tp_index)

    def tp_peer(rank):
        return (dp_index, me, rank)

    barrier = pltpu.get_barrier_semaphore()
    for rank in others:
        pl.semaphore_signal(barrier, inc=1, device_id=cp_peer(rank), device_id_type=MESH_ID)
    for shift in range(1, n_tp):
        pl.semaphore_signal(barrier, inc=1, device_id=tp_peer((tp_index + shift) % n_tp), device_id_type=MESH_ID)
    pl.semaphore_wait(barrier, n_cp - 1 + n_tp - 1)

    far_copies, pass_copies = [], []
    for num in range(pieces):
        part = pl.ds(num * rows, rows)
        far_copies.append(pltpu.make_async_remote_copy(
            src_ref=x_ref.at[part], dst_ref=x_all.at[tp_index, part], send_sem=far_send.at[num], recv_sem=far_recv.at[num],
            device_id=tp_peer(far), device_id_type=MESH_ID))
        far_copies[num].start()
        pass_copies.append(pltpu.make_async_remote_copy(
            src_ref=x_all.at[far, part], dst_ref=x_all.at[far, part], send_sem=pass_send.at[num], recv_sem=pass_recv.at[num],
            device_id=tp_peer(pair), device_id_type=MESH_ID))
    pair_copy = pltpu.make_async_remote_copy(
        src_ref=x_ref, dst_ref=x_all.at[tp_index], send_sem=pair_sem.at[0], recv_sem=pair_sem.at[1],
        device_id=tp_peer(pair), device_id_type=MESH_ID)
    pair_copy.start()

    def key_copies(step, half, rank, owner):
        k_copy = pltpu.make_async_remote_copy(
            src_ref=k_own.at[half], dst_ref=kc_all.at[owner * 2 + half], send_sem=k_send.at[step, half], recv_sem=k_recv.at[owner, half],
            device_id=cp_peer(rank), device_id_type=MESH_ID)
        at = pl.ds((owner * 2 + half) * 2, 2)
        v_copy = pltpu.make_async_remote_copy(
            src_ref=v_all.at[at], dst_ref=v_all.at[at], send_sem=v_send.at[step, half], recv_sem=v_recv.at[owner, half],
            device_id=cp_peer(rank), device_id_type=MESH_ID)
        return k_copy, v_copy

    wo_copies = [pltpu.make_async_copy(w_o_ref, w_o_all.at[0], local_sem.at[0])]
    for shift in range(1, n_tp):
        wo_copies.append(pltpu.make_async_remote_copy(
            src_ref=w_o_ref, dst_ref=w_o_all.at[shift], send_sem=wo_send.at[shift], recv_sem=wo_recv.at[shift],
            device_id=tp_peer((tp_index + shift) % n_tp), device_id_type=MESH_ID))
    ex_copies = []
    for which, (src, dst) in enumerate(((gate_ref, gate_other), (up_ref, up_other), (down_ref, down_other))):
        ex_copies.append(pltpu.make_async_remote_copy(
            src_ref=src, dst_ref=dst, send_sem=ex_send.at[which], recv_sem=ex_recv.at[which], device_id=tp_peer(pair), device_id_type=MESH_ID))

    contract = (((1,), (1,)), ((), ()))

    def project(block, start, size):
        x_blk = x_all[block, start:start + size]
        rest = lax.dot_general(w_q[...], x_blk, contract, preferred_element_type=jnp.float32).astype(jnp.bfloat16).astype(jnp.float32) * score_scale
        for term in range(3):
            part = rest.astype(jnp.bfloat16)
            for head in range(heads):
                q3_ref[block, head, term * head_dim:(term + 1) * head_dim, start:start + size] = part[head * head_dim:(head + 1) * head_dim]
            rest = rest - part.astype(jnp.float32)
        v_all[me * 4 + block, :, start:start + size] = lax.dot_general(w_v[...], x_blk, contract, preferred_element_type=jnp.float32).astype(jnp.bfloat16)
        w_kk = jnp.concatenate([w_k[...], w_k[...]], axis=0)
        k_dup[block, start:start + size, :] = lax.dot_general(x_blk, w_kk, contract, preferred_element_type=jnp.float32).astype(jnp.bfloat16)

    for block in range(n_tp):
        for head in range(heads):
            q3_ref[block, head, 3 * head_dim:, :] = jnp.zeros((depth - 3 * head_dim, blk), jnp.bfloat16)
    m_ref[...] = jnp.full(m_ref.shape, -1e30, jnp.float32)
    l_ref[...] = jnp.zeros(l_ref.shape, jnp.float32)
    acc_ref[...] = jnp.zeros(acc_ref.shape, jnp.float32)

    lane = lax.broadcasted_iota(jnp.int32, (k_own.shape[2], k_exp.shape[2]), 0)
    col = lax.broadcasted_iota(jnp.int32, (k_own.shape[2], k_exp.shape[2]), 1)
    spread = [(lane == sub * (kv_heads * head_dim) + (col // depth) * head_dim + col % head_dim).astype(jnp.bfloat16) for sub in range(2)]

    def expand(k_half, at):
        for sub in range(2):
            k_exp[at * 2 + sub] = jnp.dot(k_half, spread[sub], preferred_element_type=jnp.float32).astype(jnp.bfloat16)

    def score(head, block, at, masked):
        kv = head // grp
        scores = jnp.dot(k_exp[at, :, kv * depth:(kv + 1) * depth], q3_ref[block, head], preferred_element_type=jnp.float32)
        if masked:
            k_pos = lax.broadcasted_iota(jnp.int32, (blk, blk), 0)
            q_pos = lax.broadcasted_iota(jnp.int32, (blk, blk), 1)
            scores = jnp.where(k_pos <= q_pos, scores, -1e30)
        s_refs[head % 2][...] = scores
        old = m_ref[block, head]
        old_ref[head] = old
        m_ref[block, head] = jnp.maximum(old, jnp.max(scores, axis=0, keepdims=True))

    def mix(head, block, at):
        kv = head // grp
        top = m_ref[block, head]
        prob = jnp.exp2(s_refs[head % 2][...] - top)
        part = jnp.sum(prob.reshape(blk // 8, 8, blk), axis=0)
        mixed = jnp.dot(v_all[at, kv * head_dim:(kv + 1) * head_dim, :], prob.astype(jnp.bfloat16), preferred_element_type=jnp.float32)
        rescale = jnp.exp2(old_ref[head] - top)
        l_ref[block, head] = l_ref[block, head] * rescale + part
        acc_ref[block, head] = acc_ref[block, head] * rescale + mixed

    def run(count, place, masked):
        block, at = place(0)
        score(0, block, at, masked)

        def body(num, carry):
            block, at = place(num)
            next_block, next_at = place(num + 1 - (num + 1) // count)
            for head in range(heads):
                if head + 1 < heads:
                    score(head + 1, block, at, masked)
                else:
                    score(0, next_block, next_at, masked)
                mix(head, block, at)
            return carry

        lax.fori_loop(0, count, body, 0)

    low = lax.broadcasted_iota(jnp.int32, k_dup.shape[1:], 1) < k_dup.shape[2] // 2

    def finish_half(half):
        k_own[half] = jnp.where(low, k_dup[2 * half].astype(jnp.float32), k_dup[2 * half + 1].astype(jnp.float32)).astype(jnp.bfloat16)
        expand(k_own[half], me * 2 + half)
        for step, rank in enumerate(others):
            @pl.when((1 - half) + (me - rank + 3) // 4 > 0)
            def _():
                for copy in key_copies(step, half, rank, me):
                    copy.start()

    def send_out(block):
        shift = (block - tp_index + n_tp) % n_tp
        for head in range(heads):
            total = jnp.sum(l_ref[block, head], axis=0, keepdims=True)
            o_send[block, head * head_dim:(head + 1) * head_dim, :] = (acc_ref[block, head] / total).astype(jnp.bfloat16)

        @pl.when(shift == 0)
        def _():
            out_copy(shift, block).start()

        @pl.when(shift > 0)
        def _():
            far_out(shift, block).start()

    def out_copy(shift, block):
        return pltpu.make_async_copy(o_send.at[block], o_ref.at[shift], local_sem.at[1])

    def far_out(shift, block):
        return pltpu.make_async_remote_copy(
            src_ref=o_send.at[block], dst_ref=o_ref.at[shift], send_sem=out_send.at[shift], recv_sem=out_recv.at[shift],
            device_id=tp_peer(block), device_id_type=MESH_ID)

    for load in loads:
        load.wait()
    project(tp_index, 0, blk)
    pair_copy.wait_recv()
    project(pair, 0, blk)
    finish_half(my_half)
    run(2, lambda num: (2 * my_half + num, me * 4 + 2 * my_half + num), True)
    for num in range(pieces):
        far_copies[num].wait_recv()
        pass_copies[num].start()
        project(far, num * rows, rows)
        pass_copies[num].wait_recv()
        project(far_pair, num * rows, rows)
    far_half = 1 - my_half
    finish_half(far_half)
    for copy in wo_copies + ex_copies:
        copy.start()
    run(2, lambda num: (2 * far_half + num, me * 4 + 2 * far_half + num), True)

    def place_local(num):
        late = (num + 2) // 4
        block = (1 - late) * (1 + 2 * num) + late * (1 + num // 2)
        half = (1 - late) * num
        return block, me * 4 + half * 2 + late * (num % 2)

    run(6, place_local, False)

    def visit_rank(turn, carry):
        step, part = turn // 2, turn % 2
        rank = ((2 - step) // 2) * near + (step % 2) * mid + (step // 2) * end
        below = (me - rank + 3) // 4

        @pl.when(part == 0)
        def _():
            for copy in key_copies(0, 0, rank, rank):
                copy.wait_recv()
            expand(kc_all[rank * 2], rank * 2)

            @pl.when(rank > me)
            def _():
                for copy in key_copies(0, 1, rank, rank):
                    copy.wait_recv()
                expand(kc_all[rank * 2 + 1], rank * 2 + 1)

        def place(num):
            two = part * 2 + num // 2
            block = below * (two - 1 + 3 * (1 - (two + 3) // 4) + two // 3) + (1 - below) * (2 + part)
            half = (1 - below) * (two % 2)
            return block, rank * 4 + half * 2 + num % 2

        run(4, place, False)

        @pl.when(turn == 2 * (n_cp - 1) - 2)
        def _():
            send_out(2)
            send_out(0)

        return carry

    lax.fori_loop(0, 2 * (n_cp - 1), visit_rank, 0)
    send_out(3)
    send_out(1)

    pair_copy.wait_send()
    for num in range(pieces):
        far_copies[num].wait_send()
        pass_copies[num].wait_send()
    for step, rank in enumerate(others):
        for copy in key_copies(step, 0, rank, me):
            copy.wait_send()

        @pl.when(rank < me)
        def _():
            for copy in key_copies(step, 1, rank, me):
                copy.wait_send()

    out_copy(0, tp_index).wait()
    for shift in range(1, n_tp):
        far_out(shift, (tp_index + shift) % n_tp).wait()
    for copy in wo_copies + ex_copies:
        copy.wait()


def attention(x_loc, w_q, w_k, w_v, w_o, experts, n_cp, n_tp, head_dim):
    blk, hid = x_loc.shape
    q_depth = w_q.shape[0]
    kv_depth = w_k.shape[0]
    heads = q_depth // head_dim
    kv_heads = kv_depth // head_dim
    grp = heads // kv_heads
    depth = 128
    pieces = 4
    pairs = heads * (n_tp * blk) ** 2 * n_cp // 2
    any_spec = pl.BlockSpec(memory_space=pl.ANY)
    dma = pltpu.SemaphoreType.DMA
    return pl.pallas_call(
        functools.partial(attn_kernel, n_cp, n_tp, heads, grp, head_dim, pieces),
        out_shape=(
            jax.ShapeDtypeStruct((n_tp, q_depth, blk), jnp.bfloat16),
            jax.ShapeDtypeStruct((n_tp, q_depth, hid), jnp.bfloat16),
        ) + tuple(jax.ShapeDtypeStruct(one.shape, one.dtype) for one in experts),
        in_specs=[any_spec] * 8,
        out_specs=(any_spec,) * 5,
        scratch_shapes=[
            pltpu.VMEM((n_tp, blk, hid), jnp.bfloat16),
            pltpu.VMEM((q_depth, hid), jnp.bfloat16),
            pltpu.VMEM((kv_depth, hid), jnp.bfloat16),
            pltpu.VMEM((kv_depth, hid), jnp.bfloat16),
            pltpu.VMEM((n_tp, blk, 2 * kv_depth), jnp.bfloat16),
            pltpu.VMEM((2, blk, 2 * kv_depth), jnp.bfloat16),
            pltpu.VMEM((n_tp, heads, depth, blk), jnp.bfloat16),
            pltpu.VMEM((2 * n_cp, blk, 2 * kv_depth), jnp.bfloat16),
            pltpu.VMEM((4 * n_cp, kv_depth, blk), jnp.bfloat16),
            pltpu.VMEM((4 * n_cp, blk, kv_heads * depth), jnp.bfloat16),
            pltpu.VMEM((n_tp, heads, 1, blk), jnp.float32),
            pltpu.VMEM((heads, 1, blk), jnp.float32),
            pltpu.VMEM((n_tp, heads, 8, blk), jnp.float32),
            pltpu.VMEM((n_tp, heads, head_dim, blk), jnp.float32),
            pltpu.VMEM((blk, blk), jnp.float32),
            pltpu.VMEM((blk, blk), jnp.float32),
            pltpu.VMEM((n_tp, q_depth, blk), jnp.bfloat16),
            dma((4,)), dma((2,)), dma((pieces,)), dma((pieces,)), dma((pieces,)), dma((pieces,)),
            dma((n_cp - 1, 2)), dma((n_cp, 2)), dma((n_cp - 1, 2)), dma((n_cp, 2)), dma((2,)),
            dma((n_tp,)), dma((n_tp,)), dma((3,)), dma((3,)), dma((n_tp,)), dma((n_tp,)),
        ],
        compiler_params=pltpu.CompilerParams(collective_id=2, has_side_effects=True, vmem_limit_bytes=67043328),
        cost_estimate=pl.CostEstimate(flops=4 * pairs * 64, bytes_accessed=40 * 1024 * 1024, transcendentals=pairs),
        name="causal_attention",
    )(x_loc, w_q, w_k, w_v, w_o, *experts)


def flip_bits(index, pattern, n_bits):
    result = 0
    for bit in range(n_bits):
        digit = (index // (1 << bit)) % 2
        result = result + ((1 - digit) if (pattern >> bit) & 1 else digit) * (1 << bit)
    return result


def expert_kernel(n_chips, order, rounds, h_ref, slot_row, slot_col, gates_ref, gate_a, gate_b, up_a, up_b, down_a, down_b, y_ref,
                  send_buf, recv, w_gate, w_up, w_down, act, z_out, z_in, y_acc, y_out, load_sem, own_sem, send_sem, recv_sem, back_sem, home_sem):
    n_bits = n_chips.bit_length() - 1
    dp_index = lax.axis_index("dp")
    cp_index = lax.axis_index("cp")
    tp_index = lax.axis_index("tp")
    core = tp_index % 2
    chip = cp_index * 2 + tp_index // 2

    def peer(pattern):
        other = flip_bits(chip, pattern, n_bits)
        return (dp_index, other // 2, (other % 2) * 2 + core)

    loads = []
    for half, refs in enumerate(((gate_a, up_a, down_a), (gate_b, up_b, down_b))):
        for which, (src, dst) in enumerate(zip(refs, (w_gate, w_up, w_down))):
            loads.append(pltpu.make_async_copy(src.at[0], dst.at[half], load_sem.at[half, which]))
    for load in loads:
        load.start()
    barrier = pltpu.get_barrier_semaphore()
    for pattern in range(1, n_chips):
        pl.semaphore_signal(barrier, inc=1, device_id=peer(pattern), device_id_type=MESH_ID)
    pl.semaphore_wait(barrier, n_chips - 1)

    rows = recv.shape[1]
    hid = recv.shape[2]
    tok = h_ref.shape[0]
    ffn = w_gate.shape[2]
    tile = 256

    def pick(pattern):
        slots = lax.broadcasted_iota(jnp.int32, (rows, tok), 0) + pattern * rows
        chosen = (slots == slot_row[0:1, :]) | (slots == slot_row[1:2, :])
        return jnp.dot(chosen.astype(jnp.bfloat16), h_ref[...], preferred_element_type=jnp.float32).astype(jnp.bfloat16)

    sends = {}
    for pattern in order:
        sends[pattern] = pltpu.make_async_remote_copy(
            src_ref=send_buf.at[pattern], dst_ref=recv.at[pattern], send_sem=send_sem.at[pattern], recv_sem=recv_sem.at[pattern],
            device_id=peer(pattern), device_id_type=MESH_ID)
    late = None
    for pattern in order:
        send_buf[pattern] = pick(pattern)
        if late is not None:
            sends[late].start()
        late = pattern
    recv[0] = pick(0)
    sends[late].start()
    y_acc[...] = h_ref[...].astype(jnp.float32)

    def combine(pattern):
        slots = lax.broadcasted_iota(jnp.int32, (tok, rows), 1) + pattern * rows
        z_blk = z_in[pattern]
        for choice in range(slot_row.shape[0]):
            chosen = (slots == slot_col[:, choice:choice + 1]).astype(jnp.bfloat16)
            y_acc[...] = y_acc[...] + gates_ref[:, choice:choice + 1] * jnp.dot(chosen, z_blk, preferred_element_type=jnp.float32)

    backs = {}
    for turn, (first, second) in enumerate(rounds):
        for pattern in (first, second):
            if pattern:
                sends[pattern].wait_recv()
        for half in range(2):
            if turn == 0:
                loads[half * 3].wait()
                loads[half * 3 + 1].wait()

        x_blk = jnp.concatenate([recv[first], recv[second]], axis=0)

        def half_step(half, carry):
            for col in range(0, ffn, tile):
                gate_pre = jnp.dot(x_blk, w_gate[half, :, col:col + tile], preferred_element_type=jnp.float32)
                up_pre = jnp.dot(x_blk, w_up[half, :, col:col + tile], preferred_element_type=jnp.float32)
                act[half, :, col:col + tile] = (jax.nn.silu(gate_pre) * up_pre).astype(jnp.bfloat16)
            return carry

        lax.fori_loop(0, 2, half_step, 0)
        if turn == 0:
            for half in range(2):
                loads[half * 3 + 2].wait()

        def out_step(col, carry):
            at = pl.multiple_of(col * tile, tile)
            z_blk = jnp.dot(act[0], w_down[0, :, pl.ds(at, tile)], preferred_element_type=jnp.float32)
            z_blk = z_blk + jnp.dot(act[1], w_down[1, :, pl.ds(at, tile)], preferred_element_type=jnp.float32)
            z_blk = z_blk.astype(jnp.bfloat16)
            z_out[first, :, pl.ds(at, tile)] = z_blk[:rows]
            z_out[second, :, pl.ds(at, tile)] = z_blk[rows:]
            return carry

        lax.fori_loop(0, hid // tile, out_step, 0)
        for pattern in (first, second):
            if pattern:
                backs[pattern] = pltpu.make_async_remote_copy(
                    src_ref=z_out.at[pattern], dst_ref=z_in.at[pattern], send_sem=back_sem.at[pattern], recv_sem=home_sem.at[pattern],
                    device_id=peer(pattern), device_id_type=MESH_ID)
                backs[pattern].start()
    z_in[0] = z_out[0]
    combine(0)
    for pattern in order:
        backs[pattern].wait_recv()
        combine(pattern)
    y_out[...] = y_acc[...].astype(jnp.bfloat16)
    result = pltpu.make_async_copy(y_out, y_ref, own_sem.at[0])
    result.start()
    for pattern in order:
        sends[pattern].wait_send()
        backs[pattern].wait_send()
    result.wait()


def expert_layer(h_loc, slot_idx, gates, n_chips, own_weights, other_weights):
    tok, hid = h_loc.shape
    rows = slot_idx.shape[1] * tok // n_chips
    ffn = own_weights[0].shape[2]
    order = (1, 4, 6, 5, 7, 2, 3)
    rounds = ((0, 1), (4, 6), (5, 7), (2, 3))
    weights = []
    for own, other in zip(own_weights, other_weights):
        weights += [own, other]
    any_spec = pl.BlockSpec(memory_space=pl.ANY)
    vmem = pl.BlockSpec(memory_space=pltpu.VMEM)
    flops = 2 * 3 * n_chips * rows * hid * 2 * ffn
    return pl.pallas_call(
        functools.partial(expert_kernel, n_chips, order, rounds),
        out_shape=jax.ShapeDtypeStruct((tok, hid), jnp.bfloat16),
        in_specs=[vmem] * 4 + [any_spec] * 6,
        out_specs=any_spec,
        scratch_shapes=[
            pltpu.VMEM((n_chips, rows, hid), jnp.bfloat16),
            pltpu.VMEM((n_chips, rows, hid), jnp.bfloat16),
            pltpu.VMEM((2, hid, ffn), jnp.bfloat16),
            pltpu.VMEM((2, hid, ffn), jnp.bfloat16),
            pltpu.VMEM((2, ffn, hid), jnp.bfloat16),
            pltpu.VMEM((2, 2 * rows, ffn), jnp.bfloat16),
            pltpu.VMEM((n_chips, rows, hid), jnp.bfloat16),
            pltpu.VMEM((n_chips, rows, hid), jnp.bfloat16),
            pltpu.VMEM((tok, hid), jnp.float32),
            pltpu.VMEM((tok, hid), jnp.bfloat16),
            pltpu.SemaphoreType.DMA((2, 3)),
            pltpu.SemaphoreType.DMA((1,)),
            pltpu.SemaphoreType.DMA((n_chips,)),
            pltpu.SemaphoreType.DMA((n_chips,)),
            pltpu.SemaphoreType.DMA((n_chips,)),
            pltpu.SemaphoreType.DMA((n_chips,)),
        ],
        compiler_params=pltpu.CompilerParams(collective_id=1, has_side_effects=True, vmem_limit_bytes=58 * 1024 * 1024),
        cost_estimate=pl.CostEstimate(flops=flops, bytes_accessed=32 * 1024 * 1024, transcendentals=n_chips * rows * 2 * ffn),
        name="expert_layer",
    )(h_loc, slot_idx.T, slot_idx, gates, *weights)


def solution(mesh):
    n_cp = mesh.shape["cp"]
    n_tp = mesh.shape["tp"]
    row_spec = P(("dp", "cp", "tp"), None)
    head_spec = P(None, "tp", None)
    expert_spec = P(("cp", "tp"), None, None)

    def device_step(x_loc, w_q, w_k, w_v, w_o, ids_loc, gates_loc, w_gate, w_up, w_down):
        tok_dev, hid_dim = x_loc.shape
        top_k = ids_loc.shape[1]
        heads = w_q.shape[1]
        head_dim = w_q.shape[2]
        local_exp = w_gate.shape[0]
        n_experts = local_exp * n_cp * n_tp // 2
        capacity = top_k * tok_dev // n_experts
        chip = lax.axis_index("cp") * 2 + lax.axis_index("tp") // 2

        choice_hot = (ids_loc[:, :, None] == jnp.arange(n_experts)[None, None, :])
        token_hot = jnp.sum(choice_hot.astype(jnp.bfloat16), axis=1)
        earlier = (lax.broadcasted_iota(jnp.int32, (tok_dev, tok_dev), 0) > lax.broadcasted_iota(jnp.int32, (tok_dev, tok_dev), 1)).astype(jnp.bfloat16)
        rank_in = jnp.dot(earlier, token_hot, preferred_element_type=jnp.float32).astype(jnp.int32)
        place = rank_in + (jnp.arange(n_experts, dtype=jnp.int32) ^ chip)[None, :] * capacity
        dest_idx = jnp.sum(jnp.where(choice_hot, place[:, None, :], 0), axis=2)

        w_qkv_t = [one.transpose(1, 2, 0).reshape(-1, hid_dim) for one in (w_q, w_k, w_v)]
        out_t, w_o_all, *other_weights = attention(x_loc, *w_qkv_t, w_o.reshape(heads * head_dim, hid_dim), (w_gate, w_up, w_down), n_cp, n_tp, head_dim)
        out_t = out_t.reshape(n_tp * heads * head_dim, tok_dev)
        w_o_all = w_o_all.reshape(n_tp * heads * head_dim, hid_dim)
        attn_rows = lax.dot_general(out_t, w_o_all, (((0,), (0,)), ((), ())), preferred_element_type=jnp.float32)
        h_loc = (x_loc.astype(jnp.float32) + attn_rows).astype(jnp.bfloat16)

        return expert_layer(h_loc, dest_idx, gates_loc, n_experts, (w_gate, w_up, w_down), other_weights)

    return jax.shard_map(device_step, mesh=mesh, in_specs=(row_spec, head_spec, head_spec, head_spec, P("tp", None, None), row_spec, row_spec, expert_spec, expert_spec, expert_spec), out_specs=row_spec, check_vma=False)
```

```python
import functools
import math

import jax
import jax.numpy as jnp
from jax import lax
from jax.experimental import pallas as pl
from jax.experimental.pallas import tpu as pltpu
from jax.sharding import PartitionSpec as P


MESH_ID = pl.DeviceIdType.MESH


def attn_kernel(n_cp, n_tp, heads, grp, head_dim, pieces, x_ref, w_q_ref, w_k_ref, w_v_ref, w_o_ref, gate_ref, up_ref, down_ref,
                h_ref, gate_other, up_other, down_other,
                x_all, w_q, w_k, w_v, k_dup, k_own, q3_ref, kc_all, v_all, k_exp, m_ref, old_ref, top_ref, l_ref, acc_ref, s0_ref, s1_ref, o_send, o_all, w_o_all, h_acc, h_out,
                load_sem, pair_sem, far_send, far_recv, pass_send, pass_recv,
                k_send, k_recv, v_send, v_recv, local_sem, wo_send, wo_recv, ex_send, ex_recv, out_send, out_recv):
    dp_index = lax.axis_index("dp")
    me = lax.axis_index("cp")
    tp_index = lax.axis_index("tp")
    blk = x_ref.shape[0]
    kv_heads = heads // grp
    depth = k_exp.shape[2] // kv_heads
    score_scale = head_dim ** -0.5 * math.log2(math.e)
    s_refs = (s0_ref, s1_ref)
    near = me + 1 - 2 * (me % 2)
    mid = 2 - me // 2
    end = 3 * (1 - me // 2)
    others = (near, mid, end)
    pair = tp_index + 1 - 2 * (tp_index % 2)
    far = (tp_index + 2) % 4
    far_pair = (pair + 2) % 4
    my_half = tp_index // 2
    rows = blk // pieces

    loads = [pltpu.make_async_copy(x_ref, x_all.at[tp_index], load_sem.at[0])]
    for num, (src, dst) in enumerate(((w_q_ref, w_q), (w_k_ref, w_k), (w_v_ref, w_v))):
        loads.append(pltpu.make_async_copy(src, dst, load_sem.at[num + 1]))
    for load in loads:
        load.start()

    def cp_peer(rank):
        return (dp_index, rank, tp_index)

    def tp_peer(rank):
        return (dp_index, me, rank)

    barrier = pltpu.get_barrier_semaphore()
    for rank in others:
        pl.semaphore_signal(barrier, inc=1, device_id=cp_peer(rank), device_id_type=MESH_ID)
    for shift in range(1, n_tp):
        pl.semaphore_signal(barrier, inc=1, device_id=tp_peer((tp_index + shift) % n_tp), device_id_type=MESH_ID)
    pl.semaphore_wait(barrier, n_cp - 1 + n_tp - 1)

    far_copies, pass_copies = [], []
    for num in range(pieces):
        part = pl.ds(num * rows, rows)
        far_copies.append(pltpu.make_async_remote_copy(
            src_ref=x_ref.at[part], dst_ref=x_all.at[tp_index, part], send_sem=far_send.at[num], recv_sem=far_recv.at[num],
            device_id=tp_peer(far), device_id_type=MESH_ID))
        far_copies[num].start()
        pass_copies.append(pltpu.make_async_remote_copy(
            src_ref=x_all.at[far, part], dst_ref=x_all.at[far, part], send_sem=pass_send.at[num], recv_sem=pass_recv.at[num],
            device_id=tp_peer(pair), device_id_type=MESH_ID))
    pair_copy = pltpu.make_async_remote_copy(
        src_ref=x_ref, dst_ref=x_all.at[tp_index], send_sem=pair_sem.at[0], recv_sem=pair_sem.at[1],
        device_id=tp_peer(pair), device_id_type=MESH_ID)
    pair_copy.start()

    def key_copies(step, half, rank, owner):
        k_copy = pltpu.make_async_remote_copy(
            src_ref=k_own.at[half], dst_ref=kc_all.at[owner * 2 + half], send_sem=k_send.at[step, half], recv_sem=k_recv.at[owner, half],
            device_id=cp_peer(rank), device_id_type=MESH_ID)
        at = pl.ds((owner * 2 + half) * 2, 2)
        v_copy = pltpu.make_async_remote_copy(
            src_ref=v_all.at[at], dst_ref=v_all.at[at], send_sem=v_send.at[step, half], recv_sem=v_recv.at[owner, half],
            device_id=cp_peer(rank), device_id_type=MESH_ID)
        return k_copy, v_copy

    wo_copies = [pltpu.make_async_copy(w_o_ref, w_o_all.at[0], local_sem.at[0])]
    for shift in range(1, n_tp):
        wo_copies.append(pltpu.make_async_remote_copy(
            src_ref=w_o_ref, dst_ref=w_o_all.at[shift], send_sem=wo_send.at[shift], recv_sem=wo_recv.at[shift],
            device_id=tp_peer((tp_index + shift) % n_tp), device_id_type=MESH_ID))
    ex_copies = []
    for which, (src, dst) in enumerate(((gate_ref, gate_other), (up_ref, up_other), (down_ref, down_other))):
        ex_copies.append(pltpu.make_async_remote_copy(
            src_ref=src, dst_ref=dst, send_sem=ex_send.at[which], recv_sem=ex_recv.at[which], device_id=tp_peer(pair), device_id_type=MESH_ID))

    contract = (((1,), (1,)), ((), ()))

    def project(block, start, size):
        x_blk = x_all[block, start:start + size]
        rest = lax.dot_general(w_q[...], x_blk, contract, preferred_element_type=jnp.float32).astype(jnp.bfloat16).astype(jnp.float32) * score_scale
        for term in range(3):
            part = rest.astype(jnp.bfloat16)
            for head in range(heads):
                q3_ref[block, head, term * head_dim:(term + 1) * head_dim, start:start + size] = part[head * head_dim:(head + 1) * head_dim]
            rest = rest - part.astype(jnp.float32)
        v_all[me * 4 + block, :, start:start + size] = lax.dot_general(w_v[...], x_blk, contract, preferred_element_type=jnp.float32).astype(jnp.bfloat16)
        w_kk = jnp.concatenate([w_k[...], w_k[...]], axis=0)
        k_dup[block, start:start + size, :] = lax.dot_general(x_blk, w_kk, contract, preferred_element_type=jnp.float32).astype(jnp.bfloat16)

    for block in range(n_tp):
        for head in range(heads):
            q3_ref[block, head, 3 * head_dim:, :] = jnp.zeros((depth - 3 * head_dim, blk), jnp.bfloat16)
    m_ref[...] = jnp.full(m_ref.shape, -1e30, jnp.float32)
    l_ref[...] = jnp.zeros(l_ref.shape, jnp.float32)
    acc_ref[...] = jnp.zeros(acc_ref.shape, jnp.float32)

    lane = lax.broadcasted_iota(jnp.int32, (k_own.shape[2], k_exp.shape[2]), 0)
    col = lax.broadcasted_iota(jnp.int32, (k_own.shape[2], k_exp.shape[2]), 1)
    spread = [(lane == sub * (kv_heads * head_dim) + (col // depth) * head_dim + col % head_dim).astype(jnp.bfloat16) for sub in range(2)]

    def expand(k_half, at):
        for sub in range(2):
            k_exp[at * 2 + sub] = jnp.dot(k_half, spread[sub], preferred_element_type=jnp.float32).astype(jnp.bfloat16)

    def score(head, block, at, masked):
        kv = head // grp
        scores = jnp.dot(k_exp[at, :, kv * depth:(kv + 1) * depth], q3_ref[block, head], preferred_element_type=jnp.float32)
        if masked:
            k_pos = lax.broadcasted_iota(jnp.int32, (blk, blk), 0)
            q_pos = lax.broadcasted_iota(jnp.int32, (blk, blk), 1)
            scores = jnp.where(k_pos <= q_pos, scores, -1e30)
        s_refs[head % 2][...] = scores
        old = m_ref[block, head]
        old_ref[head] = old
        top = jnp.maximum(old, jnp.max(scores, axis=0, keepdims=True))
        top_ref[head] = top
        m_ref[block, head] = top

    def mix(head, block, at):
        kv = head // grp
        top = top_ref[head]
        prob = jnp.exp2(s_refs[head % 2][...] - top)
        part = jnp.sum(prob.reshape(blk // 8, 8, blk), axis=0)
        mixed = jnp.dot(v_all[at, kv * head_dim:(kv + 1) * head_dim, :], prob.astype(jnp.bfloat16), preferred_element_type=jnp.float32)
        rescale = jnp.exp2(old_ref[head] - top)
        l_ref[block, head] = l_ref[block, head] * rescale + part
        acc_ref[block, head] = acc_ref[block, head] * rescale + mixed

    def run(count, place, masked):
        block, at = place(0)
        score(0, block, at, masked)

        def body(num, carry):
            block, at = place(num)
            next_block, next_at = place(num + 1 - (num + 1) // count)
            for head in range(heads):
                if head + 1 < heads:
                    score(head + 1, block, at, masked)
                else:
                    score(0, next_block, next_at, masked)
                mix(head, block, at)
            return carry

        lax.fori_loop(0, count, body, 0)

    low = lax.broadcasted_iota(jnp.int32, k_dup.shape[1:], 1) < k_dup.shape[2] // 2

    def finish_half(half):
        k_own[half] = jnp.where(low, k_dup[2 * half].astype(jnp.float32), k_dup[2 * half + 1].astype(jnp.float32)).astype(jnp.bfloat16)
        expand(k_own[half], me * 2 + half)
        for step, rank in enumerate(others):
            @pl.when((1 - half) + (me - rank + 3) // 4 > 0)
            def _():
                for copy in key_copies(step, half, rank, me):
                    copy.start()

    def send_out(block):
        shift = (block - tp_index + n_tp) % n_tp
        for head in range(heads):
            total = jnp.sum(l_ref[block, head], axis=0, keepdims=True)
            o_send[block, head * head_dim:(head + 1) * head_dim, :] = (acc_ref[block, head] / total).astype(jnp.bfloat16)

        @pl.when(shift > 0)
        def _():
            far_out(shift, block).start()

    def far_out(shift, block):
        return pltpu.make_async_remote_copy(
            src_ref=o_send.at[block], dst_ref=o_all.at[shift], send_sem=out_send.at[shift], recv_sem=out_recv.at[shift],
            device_id=tp_peer(block), device_id_type=MESH_ID)

    for load in loads:
        load.wait()
    project(tp_index, 0, blk)
    pair_copy.wait_recv()
    project(pair, 0, blk)
    finish_half(my_half)
    run(2, lambda num: (2 * my_half + num, me * 4 + 2 * my_half + num), True)
    for num in range(pieces):
        far_copies[num].wait_recv()
        pass_copies[num].start()
        project(far, num * rows, rows)
        pass_copies[num].wait_recv()
        project(far_pair, num * rows, rows)
    far_half = 1 - my_half
    finish_half(far_half)
    for copy in wo_copies + ex_copies:
        copy.start()
    run(2, lambda num: (2 * far_half + num, me * 4 + 2 * far_half + num), True)

    def place_local(num):
        late = (num + 2) // 4
        block = (1 - late) * (1 + 2 * num) + late * (1 + num // 2)
        half = (1 - late) * num
        return block, me * 4 + half * 2 + late * (num % 2)

    run(6, place_local, False)

    def visit_rank(turn, carry):
        step, part = turn // 2, turn % 2
        rank = ((2 - step) // 2) * near + (step % 2) * mid + (step // 2) * end
        below = (me - rank + 3) // 4

        @pl.when(part == 0)
        def _():
            for copy in key_copies(0, 0, rank, rank):
                copy.wait_recv()
            expand(kc_all[rank * 2], rank * 2)

            @pl.when(rank > me)
            def _():
                for copy in key_copies(0, 1, rank, rank):
                    copy.wait_recv()
                expand(kc_all[rank * 2 + 1], rank * 2 + 1)

        def place(num):
            two = part * 2 + num // 2
            block = below * (two - 1 + 3 * (1 - (two + 3) // 4) + two // 3) + (1 - below) * (2 + part)
            half = (1 - below) * (two % 2)
            return block, rank * 4 + half * 2 + num % 2

        run(4, place, False)

        @pl.when(turn == 2 * (n_cp - 1) - 2)
        def _():
            send_out(2)
            send_out(0)

        return carry

    lax.fori_loop(0, 2 * (n_cp - 1), visit_rank, 0)
    send_out(3)
    send_out(1)

    pair_copy.wait_send()
    for num in range(pieces):
        far_copies[num].wait_send()
        pass_copies[num].wait_send()
    for step, rank in enumerate(others):
        for copy in key_copies(step, 0, rank, me):
            copy.wait_send()

        @pl.when(rank < me)
        def _():
            for copy in key_copies(step, 1, rank, me):
                copy.wait_send()

    wo_copies[0].wait()
    for shift in (0, 1, 3, 2):
        if shift:
            far_out(shift, (tp_index + shift) % n_tp).wait()
            wo_copies[shift].wait()
            o_blk = o_all[shift]
        else:
            o_blk = o_send[tp_index]
        h_part = lax.dot_general(o_blk, w_o_all[shift], (((0,), (0,)), ((), ())), preferred_element_type=jnp.float32)
        h_acc[...] = h_acc[...] + h_part if shift else h_part
    h_out[...] = (x_all[tp_index].astype(jnp.float32) + h_acc[...]).astype(jnp.bfloat16)
    result = pltpu.make_async_copy(h_out, h_ref, local_sem.at[1])
    result.start()
    for copy in ex_copies:
        copy.wait()
    result.wait()


def attention(x_loc, w_q, w_k, w_v, w_o, experts, n_cp, n_tp, head_dim):
    blk, hid = x_loc.shape
    q_depth = w_q.shape[0]
    kv_depth = w_k.shape[0]
    heads = q_depth // head_dim
    kv_heads = kv_depth // head_dim
    grp = heads // kv_heads
    depth = 128
    pieces = 4
    pairs = heads * (n_tp * blk) ** 2 * n_cp // 2
    any_spec = pl.BlockSpec(memory_space=pl.ANY)
    dma = pltpu.SemaphoreType.DMA
    return pl.pallas_call(
        functools.partial(attn_kernel, n_cp, n_tp, heads, grp, head_dim, pieces),
        out_shape=(
            jax.ShapeDtypeStruct((blk, hid), jnp.bfloat16),
        ) + tuple(jax.ShapeDtypeStruct(one.shape, one.dtype) for one in experts),
        in_specs=[any_spec] * 8,
        out_specs=(any_spec,) * 4,
        scratch_shapes=[
            pltpu.VMEM((n_tp, blk, hid), jnp.bfloat16),
            pltpu.VMEM((q_depth, hid), jnp.bfloat16),
            pltpu.VMEM((kv_depth, hid), jnp.bfloat16),
            pltpu.VMEM((kv_depth, hid), jnp.bfloat16),
            pltpu.VMEM((n_tp, blk, 2 * kv_depth), jnp.bfloat16),
            pltpu.VMEM((2, blk, 2 * kv_depth), jnp.bfloat16),
            pltpu.VMEM((n_tp, heads, depth, blk), jnp.bfloat16),
            pltpu.VMEM((2 * n_cp, blk, 2 * kv_depth), jnp.bfloat16),
            pltpu.VMEM((4 * n_cp, kv_depth, blk), jnp.bfloat16),
            pltpu.VMEM((4 * n_cp, blk, kv_heads * depth), jnp.bfloat16),
            pltpu.VMEM((n_tp, heads, 1, blk), jnp.float32),
            pltpu.VMEM((heads, 1, blk), jnp.float32),
            pltpu.VMEM((heads, 1, blk), jnp.float32),
            pltpu.VMEM((n_tp, heads, 8, blk), jnp.float32),
            pltpu.VMEM((n_tp, heads, head_dim, blk), jnp.float32),
            pltpu.VMEM((blk, blk), jnp.float32),
            pltpu.VMEM((blk, blk), jnp.float32),
            pltpu.VMEM((n_tp, q_depth, blk), jnp.bfloat16),
            pltpu.VMEM((n_tp, q_depth, blk), jnp.bfloat16),
            pltpu.VMEM((n_tp, q_depth, hid), jnp.bfloat16),
            pltpu.VMEM((blk, hid), jnp.float32),
            pltpu.VMEM((blk, hid), jnp.bfloat16),
            dma((4,)), dma((2,)), dma((pieces,)), dma((pieces,)), dma((pieces,)), dma((pieces,)),
            dma((n_cp - 1, 2)), dma((n_cp, 2)), dma((n_cp - 1, 2)), dma((n_cp, 2)), dma((2,)),
            dma((n_tp,)), dma((n_tp,)), dma((3,)), dma((3,)), dma((n_tp,)), dma((n_tp,)),
        ],
        compiler_params=pltpu.CompilerParams(collective_id=2, has_side_effects=True, vmem_limit_bytes=67043328),
        cost_estimate=pl.CostEstimate(flops=4 * pairs * 64, bytes_accessed=40 * 1024 * 1024, transcendentals=pairs),
        name="causal_attention",
    )(x_loc, w_q, w_k, w_v, w_o, *experts)


def flip_bits(index, pattern, n_bits):
    result = 0
    for bit in range(n_bits):
        digit = (index // (1 << bit)) % 2
        result = result + ((1 - digit) if (pattern >> bit) & 1 else digit) * (1 << bit)
    return result


def expert_kernel(n_chips, order, rounds, h_ref, slot_row, gate_row, gate_a, gate_b, up_a, up_b, down_a, down_b, y_ref,
                  send_buf, recv, w_gate, w_up, w_down, act, z_out, z_in, y_acc, load_sem, own_sem, send_sem, recv_sem, back_sem, home_sem):
    n_bits = n_chips.bit_length() - 1
    dp_index = lax.axis_index("dp")
    cp_index = lax.axis_index("cp")
    tp_index = lax.axis_index("tp")
    core = tp_index % 2
    chip = cp_index * 2 + tp_index // 2

    def peer(pattern):
        other = flip_bits(chip, pattern, n_bits)
        return (dp_index, other // 2, (other % 2) * 2 + core)

    loads = []
    for half, refs in enumerate(((gate_a, up_a, down_a), (gate_b, up_b, down_b))):
        for which, (src, dst) in enumerate(zip(refs, (w_gate, w_up, w_down))):
            loads.append(pltpu.make_async_copy(src.at[0], dst.at[half], load_sem.at[half, which]))
    for load in loads:
        load.start()
    barrier = pltpu.get_barrier_semaphore()
    for pattern in range(1, n_chips):
        pl.semaphore_signal(barrier, inc=1, device_id=peer(pattern), device_id_type=MESH_ID)
    pl.semaphore_wait(barrier, n_chips - 1)

    rows = recv.shape[1]
    hid = recv.shape[2]
    tok = h_ref.shape[0]
    ffn = w_gate.shape[2]
    tile = 256

    def pick(pattern):
        slots = lax.broadcasted_iota(jnp.int32, (rows, tok), 0) + pattern * rows
        chosen = (slots == slot_row[0:1, :]) | (slots == slot_row[1:2, :])
        return jnp.dot(chosen.astype(jnp.bfloat16), h_ref[...], preferred_element_type=jnp.float32).astype(jnp.bfloat16)

    sends = {}
    for pattern in order:
        sends[pattern] = pltpu.make_async_remote_copy(
            src_ref=send_buf.at[pattern], dst_ref=recv.at[pattern], send_sem=send_sem.at[pattern], recv_sem=recv_sem.at[pattern],
            device_id=peer(pattern), device_id_type=MESH_ID)
    late = None
    for pattern in order:
        send_buf[pattern] = pick(pattern)
        if late is not None:
            sends[late].start()
        late = pattern
    recv[0] = pick(0)
    sends[late].start()
    y_acc[...] = h_ref[...].astype(jnp.float32)
    by_token = jnp.concatenate([slot_row[...].astype(jnp.float32), gate_row[...], jnp.zeros((8 - 2 * slot_row.shape[0], tok), jnp.float32)], axis=0).T

    def combine(pattern):
        slots = (lax.broadcasted_iota(jnp.int32, (tok, rows), 1) + pattern * rows).astype(jnp.float32)
        z_blk = z_in[pattern]
        for choice in range(slot_row.shape[0]):
            chosen = (slots == by_token[:, choice:choice + 1]).astype(jnp.bfloat16)
            y_acc[...] = y_acc[...] + by_token[:, slot_row.shape[0] + choice:slot_row.shape[0] + choice + 1] * jnp.dot(chosen, z_blk, preferred_element_type=jnp.float32)

    backs = {}
    for turn, (first, second) in enumerate(rounds):
        for pattern in (first, second):
            if pattern:
                sends[pattern].wait_recv()
        for half in range(2):
            if turn == 0:
                loads[half * 3].wait()
                loads[half * 3 + 1].wait()

        x_blk = jnp.concatenate([recv[first], recv[second]], axis=0)

        def half_step(half, carry):
            for col in range(0, ffn, tile):
                gate_pre = jnp.dot(x_blk, w_gate[half, :, col:col + tile], preferred_element_type=jnp.float32)
                up_pre = jnp.dot(x_blk, w_up[half, :, col:col + tile], preferred_element_type=jnp.float32)
                act[half, :, col:col + tile] = (jax.nn.silu(gate_pre) * up_pre).astype(jnp.bfloat16)
            return carry

        lax.fori_loop(0, 2, half_step, 0)
        if turn == 0:
            for half in range(2):
                loads[half * 3 + 2].wait()

        def out_step(col, carry):
            at = pl.multiple_of(col * tile, tile)
            z_blk = jnp.dot(act[0], w_down[0, :, pl.ds(at, tile)], preferred_element_type=jnp.float32)
            z_blk = z_blk + jnp.dot(act[1], w_down[1, :, pl.ds(at, tile)], preferred_element_type=jnp.float32)
            z_blk = z_blk.astype(jnp.bfloat16)
            z_out[first, :, pl.ds(at, tile)] = z_blk[:rows]
            z_out[second, :, pl.ds(at, tile)] = z_blk[rows:]
            return carry

        lax.fori_loop(0, hid // tile, out_step, 0)
        for pattern in (first, second):
            if pattern:
                backs[pattern] = pltpu.make_async_remote_copy(
                    src_ref=z_out.at[pattern], dst_ref=z_in.at[pattern], send_sem=back_sem.at[pattern], recv_sem=home_sem.at[pattern],
                    device_id=peer(pattern), device_id_type=MESH_ID)
                backs[pattern].start()
    z_in[0] = z_out[0]
    combine(0)
    for pattern in order:
        backs[pattern].wait_recv()
        combine(pattern)
    result = pltpu.make_async_copy(y_acc, y_ref, own_sem.at[0])
    result.start()
    for pattern in order:
        sends[pattern].wait_send()
        backs[pattern].wait_send()
    result.wait()


def expert_layer(h_loc, slot_idx, gates, n_chips, own_weights, other_weights):
    tok, hid = h_loc.shape
    rows = slot_idx.shape[1] * tok // n_chips
    ffn = own_weights[0].shape[2]
    order = (1, 4, 6, 5, 7, 2, 3)
    rounds = ((0, 1), (4, 6), (5, 7), (2, 3))
    weights = []
    for own, other in zip(own_weights, other_weights):
        weights += [own, other]
    any_spec = pl.BlockSpec(memory_space=pl.ANY)
    vmem = pl.BlockSpec(memory_space=pltpu.VMEM)
    flops = 2 * 3 * n_chips * rows * hid * 2 * ffn
    return pl.pallas_call(
        functools.partial(expert_kernel, n_chips, order, rounds),
        out_shape=jax.ShapeDtypeStruct((tok, hid), jnp.float32),
        in_specs=[vmem] * 3 + [any_spec] * 6,
        out_specs=any_spec,
        scratch_shapes=[
            pltpu.VMEM((n_chips, rows, hid), jnp.bfloat16),
            pltpu.VMEM((n_chips, rows, hid), jnp.bfloat16),
            pltpu.VMEM((2, hid, ffn), jnp.bfloat16),
            pltpu.VMEM((2, hid, ffn), jnp.bfloat16),
            pltpu.VMEM((2, ffn, hid), jnp.bfloat16),
            pltpu.VMEM((2, 2 * rows, ffn), jnp.bfloat16),
            pltpu.VMEM((n_chips, rows, hid), jnp.bfloat16),
            pltpu.VMEM((n_chips, rows, hid), jnp.bfloat16),
            pltpu.VMEM((tok, hid), jnp.float32),
            pltpu.SemaphoreType.DMA((2, 3)),
            pltpu.SemaphoreType.DMA((1,)),
            pltpu.SemaphoreType.DMA((n_chips,)),
            pltpu.SemaphoreType.DMA((n_chips,)),
            pltpu.SemaphoreType.DMA((n_chips,)),
            pltpu.SemaphoreType.DMA((n_chips,)),
        ],
        compiler_params=pltpu.CompilerParams(collective_id=1, has_side_effects=True, vmem_limit_bytes=58 * 1024 * 1024),
        cost_estimate=pl.CostEstimate(flops=flops, bytes_accessed=32 * 1024 * 1024, transcendentals=n_chips * rows * 2 * ffn),
        name="expert_layer",
    )(h_loc, slot_idx.T, gates.T, *weights)


def solution(mesh):
    n_cp = mesh.shape["cp"]
    n_tp = mesh.shape["tp"]
    row_spec = P(("dp", "cp", "tp"), None)
    head_spec = P(None, "tp", None)
    expert_spec = P(("cp", "tp"), None, None)

    def device_step(x_loc, w_q, w_k, w_v, w_o, ids_loc, gates_loc, w_gate, w_up, w_down):
        tok_dev, hid_dim = x_loc.shape
        top_k = ids_loc.shape[1]
        heads = w_q.shape[1]
        head_dim = w_q.shape[2]
        local_exp = w_gate.shape[0]
        n_experts = local_exp * n_cp * n_tp // 2
        capacity = top_k * tok_dev // n_experts
        chip = lax.axis_index("cp") * 2 + lax.axis_index("tp") // 2

        choice_hot = (ids_loc[:, :, None] == jnp.arange(n_experts)[None, None, :])
        token_hot = jnp.sum(choice_hot.astype(jnp.bfloat16), axis=1)
        earlier = (lax.broadcasted_iota(jnp.int32, (tok_dev, tok_dev), 0) > lax.broadcasted_iota(jnp.int32, (tok_dev, tok_dev), 1)).astype(jnp.bfloat16)
        rank_in = jnp.dot(earlier, token_hot, preferred_element_type=jnp.float32).astype(jnp.int32)
        place = rank_in + (jnp.arange(n_experts, dtype=jnp.int32) ^ chip)[None, :] * capacity
        dest_idx = jnp.sum(jnp.where(choice_hot, place[:, None, :], 0), axis=2)

        w_qkv_t = [one.transpose(1, 2, 0).reshape(-1, hid_dim) for one in (w_q, w_k, w_v)]
        h_loc, *other_weights = attention(x_loc, *w_qkv_t, w_o.reshape(heads * head_dim, hid_dim), (w_gate, w_up, w_down), n_cp, n_tp, head_dim)
        return expert_layer(h_loc, dest_idx, gates_loc, n_experts, (w_gate, w_up, w_down), other_weights).astype(jnp.bfloat16)

    return jax.shard_map(device_step, mesh=mesh, in_specs=(row_spec, head_spec, head_spec, head_spec, P("tp", None, None), row_spec, row_spec, expert_spec, expert_spec, expert_spec), out_specs=row_spec, check_vma=False)
```

```python
import functools
import math

import jax
import jax.numpy as jnp
from jax import lax
from jax.experimental import pallas as pl
from jax.experimental.pallas import tpu as pltpu
from jax.sharding import PartitionSpec as P


MESH_ID = pl.DeviceIdType.MESH


def attn_kernel(n_cp, n_tp, heads, grp, head_dim, pieces, x_ref, w_q_ref, w_k_ref, w_v_ref, w_o_ref, gate_ref, up_ref, down_ref,
                h_ref, gate_other, up_other, down_other,
                x_all, w_q, w_k, w_v, k_dup, k_own, q3_ref, kc_all, v_all, k_exp, m_ref, old_ref, top_ref, l_ref, acc_ref, s0_ref, s1_ref, o_send, o_all, w_o_all, h_acc, h_out,
                load_sem, pair_sem, far_send, far_recv, pass_send, pass_recv,
                k_send, k_recv, v_send, v_recv, local_sem, wo_send, wo_recv, ex_send, ex_recv, out_send, out_recv):
    dp_index = lax.axis_index("dp")
    me = lax.axis_index("cp")
    tp_index = lax.axis_index("tp")
    blk = x_ref.shape[0]
    kv_heads = heads // grp
    depth = k_exp.shape[2] // kv_heads
    score_scale = head_dim ** -0.5 * math.log2(math.e)
    s_refs = (s0_ref, s1_ref)
    near = me + 1 - 2 * (me % 2)
    mid = 2 - me // 2
    end = 3 * (1 - me // 2)
    others = (near, mid, end)
    pair = tp_index + 1 - 2 * (tp_index % 2)
    far = (tp_index + 2) % 4
    far_pair = (pair + 2) % 4
    my_half = tp_index // 2
    rows = blk // pieces

    loads = [pltpu.make_async_copy(x_ref, x_all.at[tp_index], load_sem.at[0])]
    for num, (src, dst) in enumerate(((w_q_ref, w_q), (w_k_ref, w_k), (w_v_ref, w_v))):
        loads.append(pltpu.make_async_copy(src, dst, load_sem.at[num + 1]))
    for load in loads:
        load.start()

    def cp_peer(rank):
        return (dp_index, rank, tp_index)

    def tp_peer(rank):
        return (dp_index, me, rank)

    barrier = pltpu.get_barrier_semaphore()
    for rank in others:
        pl.semaphore_signal(barrier, inc=1, device_id=cp_peer(rank), device_id_type=MESH_ID)
    for shift in range(1, n_tp):
        pl.semaphore_signal(barrier, inc=1, device_id=tp_peer((tp_index + shift) % n_tp), device_id_type=MESH_ID)
    pl.semaphore_wait(barrier, n_cp - 1 + n_tp - 1)

    far_copies, pass_copies = [], []
    for num in range(pieces):
        part = pl.ds(num * rows, rows)
        far_copies.append(pltpu.make_async_remote_copy(
            src_ref=x_ref.at[part], dst_ref=x_all.at[tp_index, part], send_sem=far_send.at[num], recv_sem=far_recv.at[num],
            device_id=tp_peer(far), device_id_type=MESH_ID))
        far_copies[num].start()
        pass_copies.append(pltpu.make_async_remote_copy(
            src_ref=x_all.at[far, part], dst_ref=x_all.at[far, part], send_sem=pass_send.at[num], recv_sem=pass_recv.at[num],
            device_id=tp_peer(pair), device_id_type=MESH_ID))
    pair_copy = pltpu.make_async_remote_copy(
        src_ref=x_ref, dst_ref=x_all.at[tp_index], send_sem=pair_sem.at[0], recv_sem=pair_sem.at[1],
        device_id=tp_peer(pair), device_id_type=MESH_ID)
    pair_copy.start()

    def key_copies(step, half, rank, owner):
        k_copy = pltpu.make_async_remote_copy(
            src_ref=k_own.at[half], dst_ref=kc_all.at[owner * 2 + half], send_sem=k_send.at[step, half], recv_sem=k_recv.at[owner, half],
            device_id=cp_peer(rank), device_id_type=MESH_ID)
        at = pl.ds((owner * 2 + half) * 2, 2)
        v_copy = pltpu.make_async_remote_copy(
            src_ref=v_all.at[at], dst_ref=v_all.at[at], send_sem=v_send.at[step, half], recv_sem=v_recv.at[owner, half],
            device_id=cp_peer(rank), device_id_type=MESH_ID)
        return k_copy, v_copy

    wo_copies = [pltpu.make_async_copy(w_o_ref, w_o_all.at[0], local_sem.at[0])]
    for shift in range(1, n_tp):
        wo_copies.append(pltpu.make_async_remote_copy(
            src_ref=w_o_ref, dst_ref=w_o_all.at[shift], send_sem=wo_send.at[shift], recv_sem=wo_recv.at[shift],
            device_id=tp_peer((tp_index + shift) % n_tp), device_id_type=MESH_ID))
    ex_copies = []
    for which, (src, dst) in enumerate(((gate_ref, gate_other), (up_ref, up_other), (down_ref, down_other))):
        ex_copies.append(pltpu.make_async_remote_copy(
            src_ref=src, dst_ref=dst, send_sem=ex_send.at[which], recv_sem=ex_recv.at[which], device_id=tp_peer(pair), device_id_type=MESH_ID))

    contract = (((1,), (1,)), ((), ()))

    def project(block, start, size):
        x_blk = x_all[block, start:start + size]
        rest = lax.dot_general(w_q[...], x_blk, contract, preferred_element_type=jnp.float32).astype(jnp.bfloat16).astype(jnp.float32) * score_scale
        for term in range(3):
            part = rest.astype(jnp.bfloat16)
            for head in range(heads):
                q3_ref[block, head, term * head_dim:(term + 1) * head_dim, start:start + size] = part[head * head_dim:(head + 1) * head_dim]
            rest = rest - part.astype(jnp.float32)
        v_all[me * 4 + block, :, start:start + size] = lax.dot_general(w_v[...], x_blk, contract, preferred_element_type=jnp.float32).astype(jnp.bfloat16)
        w_kk = jnp.concatenate([w_k[...], w_k[...]], axis=0)
        k_dup[block, start:start + size, :] = lax.dot_general(x_blk, w_kk, contract, preferred_element_type=jnp.float32).astype(jnp.bfloat16)

    for block in range(n_tp):
        for head in range(heads):
            q3_ref[block, head, 3 * head_dim:, :] = jnp.zeros((depth - 3 * head_dim, blk), jnp.bfloat16)
    m_ref[...] = jnp.full(m_ref.shape, -1e30, jnp.float32)
    l_ref[...] = jnp.zeros(l_ref.shape, jnp.float32)
    acc_ref[...] = jnp.zeros(acc_ref.shape, jnp.float32)

    lane = lax.broadcasted_iota(jnp.int32, (k_own.shape[2], k_exp.shape[2]), 0)
    col = lax.broadcasted_iota(jnp.int32, (k_own.shape[2], k_exp.shape[2]), 1)
    spread = [(lane == sub * (kv_heads * head_dim) + (col // depth) * head_dim + col % head_dim).astype(jnp.bfloat16) for sub in range(2)]

    def expand(k_half, at):
        for sub in range(2):
            k_exp[at * 2 + sub] = jnp.dot(k_half, spread[sub], preferred_element_type=jnp.float32).astype(jnp.bfloat16)

    def score(head, block, at, masked):
        kv = head // grp
        scores = jnp.dot(k_exp[at, :, kv * depth:(kv + 1) * depth], q3_ref[block, head], preferred_element_type=jnp.float32)
        if masked:
            k_pos = lax.broadcasted_iota(jnp.int32, (blk, blk), 0)
            q_pos = lax.broadcasted_iota(jnp.int32, (blk, blk), 1)
            scores = jnp.where(k_pos <= q_pos, scores, -1e30)
        s_refs[head % 2][...] = scores
        old = m_ref[block, head]
        old_ref[head] = old
        top = jnp.maximum(old, jnp.max(scores, axis=0, keepdims=True))
        top_ref[head] = top
        m_ref[block, head] = top

    def mix(head, block, at):
        kv = head // grp
        top = top_ref[head]
        prob = jnp.exp2(s_refs[head % 2][...] - top)
        part = jnp.sum(prob.reshape(blk // 8, 8, blk), axis=0)
        mixed = jnp.dot(v_all[at, kv * head_dim:(kv + 1) * head_dim, :], prob.astype(jnp.bfloat16), preferred_element_type=jnp.float32)
        rescale = jnp.exp2(old_ref[head] - top)
        l_ref[block, head] = l_ref[block, head] * rescale + part
        acc_ref[block, head] = acc_ref[block, head] * rescale + mixed

    def run(count, place, masked):
        block, at = place(0)
        score(0, block, at, masked)

        def body(num, carry):
            block, at = place(num)
            next_block, next_at = place(num + 1 - (num + 1) // count)
            for head in range(heads):
                if head + 1 < heads:
                    score(head + 1, block, at, masked)
                else:
                    score(0, next_block, next_at, masked)
                mix(head, block, at)
            return carry

        lax.fori_loop(0, count, body, 0)

    low = lax.broadcasted_iota(jnp.int32, k_dup.shape[1:], 1) < k_dup.shape[2] // 2

    def finish_half(half):
        k_own[half] = jnp.where(low, k_dup[2 * half].astype(jnp.float32), k_dup[2 * half + 1].astype(jnp.float32)).astype(jnp.bfloat16)
        expand(k_own[half], me * 2 + half)
        for step, rank in enumerate(others):
            @pl.when((1 - half) + (me - rank + 3) // 4 > 0)
            def _():
                for copy in key_copies(step, half, rank, me):
                    copy.start()

    def send_out(block):
        shift = (block - tp_index + n_tp) % n_tp
        for head in range(heads):
            total = jnp.sum(l_ref[block, head], axis=0, keepdims=True)
            o_send[block, head * head_dim:(head + 1) * head_dim, :] = (acc_ref[block, head] / total).astype(jnp.bfloat16)

        @pl.when(shift > 0)
        def _():
            far_out(shift, block).start()

    def far_out(shift, block):
        return pltpu.make_async_remote_copy(
            src_ref=o_send.at[block], dst_ref=o_all.at[shift], send_sem=out_send.at[shift], recv_sem=out_recv.at[shift],
            device_id=tp_peer(block), device_id_type=MESH_ID)

    for load in loads:
        load.wait()
    project(tp_index, 0, blk)
    pair_copy.wait_recv()
    project(pair, 0, blk)
    finish_half(my_half)
    run(2, lambda num: (2 * my_half + num, me * 4 + 2 * my_half + num), True)
    run(1, lambda num: (2 * my_half + 1, me * 4 + 2 * my_half), False)
    for num in range(pieces):
        far_copies[num].wait_recv()
        pass_copies[num].start()
        project(far, num * rows, rows)
        pass_copies[num].wait_recv()
        project(far_pair, num * rows, rows)
    far_half = 1 - my_half
    finish_half(far_half)
    for copy in wo_copies + ex_copies:
        copy.start()
    run(2, lambda num: (2 * far_half + num, me * 4 + 2 * far_half + num), True)

    def place_local(num):
        late = (num + 4) // 5
        block = (1 - late) * (2 * far_half + 1) + late * (1 + (num + 1) // 2)
        at = (1 - late) * 2 * far_half + late * ((num + 1) % 2)
        return block, me * 4 + at

    run(5, place_local, False)

    def visit_rank(turn, carry):
        step, part = turn // 2, turn % 2
        rank = ((2 - step) // 2) * near + (step % 2) * mid + (step // 2) * end
        below = (me - rank + 3) // 4

        @pl.when(part == 0)
        def _():
            for copy in key_copies(0, 0, rank, rank):
                copy.wait_recv()
            expand(kc_all[rank * 2], rank * 2)

            @pl.when(rank > me)
            def _():
                for copy in key_copies(0, 1, rank, rank):
                    copy.wait_recv()
                expand(kc_all[rank * 2 + 1], rank * 2 + 1)

        def place(num):
            two = part * 2 + num // 2
            block = below * (two - 1 + 3 * (1 - (two + 3) // 4) + two // 3) + (1 - below) * (2 + part)
            half = (1 - below) * (two % 2)
            return block, rank * 4 + half * 2 + num % 2

        run(4, place, False)

        @pl.when(turn == 2 * (n_cp - 1) - 2)
        def _():
            send_out(2)
            send_out(0)

        return carry

    lax.fori_loop(0, 2 * (n_cp - 1), visit_rank, 0)
    send_out(3)
    send_out(1)

    pair_copy.wait_send()
    for num in range(pieces):
        far_copies[num].wait_send()
        pass_copies[num].wait_send()
    for step, rank in enumerate(others):
        for copy in key_copies(step, 0, rank, me):
            copy.wait_send()

        @pl.when(rank < me)
        def _():
            for copy in key_copies(step, 1, rank, me):
                copy.wait_send()

    wo_copies[0].wait()
    for shift in (0, 1, 3, 2):
        if shift:
            far_out(shift, (tp_index + shift) % n_tp).wait()
            wo_copies[shift].wait()
            o_blk = o_all[shift]
        else:
            o_blk = o_send[tp_index]
        h_part = lax.dot_general(o_blk, w_o_all[shift], (((0,), (0,)), ((), ())), preferred_element_type=jnp.float32)
        h_acc[...] = h_acc[...] + h_part if shift else h_part
    h_out[...] = (x_all[tp_index].astype(jnp.float32) + h_acc[...]).astype(jnp.bfloat16)
    result = pltpu.make_async_copy(h_out, h_ref, local_sem.at[1])
    result.start()
    for copy in ex_copies:
        copy.wait()
    result.wait()


def attention(x_loc, w_q, w_k, w_v, w_o, experts, n_cp, n_tp, head_dim):
    blk, hid = x_loc.shape
    q_depth = w_q.shape[0]
    kv_depth = w_k.shape[0]
    heads = q_depth // head_dim
    kv_heads = kv_depth // head_dim
    grp = heads // kv_heads
    depth = 128
    pieces = 4
    pairs = heads * (n_tp * blk) ** 2 * n_cp // 2
    any_spec = pl.BlockSpec(memory_space=pl.ANY)
    dma = pltpu.SemaphoreType.DMA
    return pl.pallas_call(
        functools.partial(attn_kernel, n_cp, n_tp, heads, grp, head_dim, pieces),
        out_shape=(
            jax.ShapeDtypeStruct((blk, hid), jnp.bfloat16),
        ) + tuple(jax.ShapeDtypeStruct(one.shape, one.dtype) for one in experts),
        in_specs=[any_spec] * 8,
        out_specs=(any_spec,) * 4,
        scratch_shapes=[
            pltpu.VMEM((n_tp, blk, hid), jnp.bfloat16),
            pltpu.VMEM((q_depth, hid), jnp.bfloat16),
            pltpu.VMEM((kv_depth, hid), jnp.bfloat16),
            pltpu.VMEM((kv_depth, hid), jnp.bfloat16),
            pltpu.VMEM((n_tp, blk, 2 * kv_depth), jnp.bfloat16),
            pltpu.VMEM((2, blk, 2 * kv_depth), jnp.bfloat16),
            pltpu.VMEM((n_tp, heads, depth, blk), jnp.bfloat16),
            pltpu.VMEM((2 * n_cp, blk, 2 * kv_depth), jnp.bfloat16),
            pltpu.VMEM((4 * n_cp, kv_depth, blk), jnp.bfloat16),
            pltpu.VMEM((4 * n_cp, blk, kv_heads * depth), jnp.bfloat16),
            pltpu.VMEM((n_tp, heads, 1, blk), jnp.float32),
            pltpu.VMEM((heads, 1, blk), jnp.float32),
            pltpu.VMEM((heads, 1, blk), jnp.float32),
            pltpu.VMEM((n_tp, heads, 8, blk), jnp.float32),
            pltpu.VMEM((n_tp, heads, head_dim, blk), jnp.float32),
            pltpu.VMEM((blk, blk), jnp.float32),
            pltpu.VMEM((blk, blk), jnp.float32),
            pltpu.VMEM((n_tp, q_depth, blk), jnp.bfloat16),
            pltpu.VMEM((n_tp, q_depth, blk), jnp.bfloat16),
            pltpu.VMEM((n_tp, q_depth, hid), jnp.bfloat16),
            pltpu.VMEM((blk, hid), jnp.float32),
            pltpu.VMEM((blk, hid), jnp.bfloat16),
            dma((4,)), dma((2,)), dma((pieces,)), dma((pieces,)), dma((pieces,)), dma((pieces,)),
            dma((n_cp - 1, 2)), dma((n_cp, 2)), dma((n_cp - 1, 2)), dma((n_cp, 2)), dma((2,)),
            dma((n_tp,)), dma((n_tp,)), dma((3,)), dma((3,)), dma((n_tp,)), dma((n_tp,)),
        ],
        compiler_params=pltpu.CompilerParams(collective_id=2, has_side_effects=True, vmem_limit_bytes=67043328),
        cost_estimate=pl.CostEstimate(flops=4 * pairs * 64, bytes_accessed=40 * 1024 * 1024, transcendentals=pairs),
        name="causal_attention",
    )(x_loc, w_q, w_k, w_v, w_o, *experts)


def flip_bits(index, pattern, n_bits):
    result = 0
    for bit in range(n_bits):
        digit = (index // (1 << bit)) % 2
        result = result + ((1 - digit) if (pattern >> bit) & 1 else digit) * (1 << bit)
    return result


def expert_kernel(n_chips, order, rounds, h_ref, slot_row, gate_row, gate_a, gate_b, up_a, up_b, down_a, down_b, y_ref,
                  send_buf, recv, w_gate, w_up, w_down, act, z_out, z_in, y_acc, load_sem, own_sem, send_sem, recv_sem, back_sem, home_sem):
    n_bits = n_chips.bit_length() - 1
    dp_index = lax.axis_index("dp")
    cp_index = lax.axis_index("cp")
    tp_index = lax.axis_index("tp")
    core = tp_index % 2
    chip = cp_index * 2 + tp_index // 2

    def peer(pattern):
        other = flip_bits(chip, pattern, n_bits)
        return (dp_index, other // 2, (other % 2) * 2 + core)

    loads = []
    for half, refs in enumerate(((gate_a, up_a, down_a), (gate_b, up_b, down_b))):
        for which, (src, dst) in enumerate(zip(refs, (w_gate, w_up, w_down))):
            loads.append(pltpu.make_async_copy(src.at[0], dst.at[half], load_sem.at[half, which]))
    for load in loads:
        load.start()
    barrier = pltpu.get_barrier_semaphore()
    for pattern in range(1, n_chips):
        pl.semaphore_signal(barrier, inc=1, device_id=peer(pattern), device_id_type=MESH_ID)
    pl.semaphore_wait(barrier, n_chips - 1)

    rows = recv.shape[1]
    hid = recv.shape[2]
    tok = h_ref.shape[0]
    ffn = w_gate.shape[2]
    tile = 256

    def pick(pattern):
        slots = lax.broadcasted_iota(jnp.int32, (rows, tok), 0) + pattern * rows
        chosen = (slots == slot_row[0:1, :]) | (slots == slot_row[1:2, :])
        return jnp.dot(chosen.astype(jnp.bfloat16), h_ref[...], preferred_element_type=jnp.float32).astype(jnp.bfloat16)

    sends = {}
    for pattern in order:
        sends[pattern] = pltpu.make_async_remote_copy(
            src_ref=send_buf.at[pattern], dst_ref=recv.at[pattern], send_sem=send_sem.at[pattern], recv_sem=recv_sem.at[pattern],
            device_id=peer(pattern), device_id_type=MESH_ID)
    late = None
    for pattern in order:
        send_buf[pattern] = pick(pattern)
        if late is not None:
            sends[late].start()
        late = pattern
    recv[0] = pick(0)
    sends[late].start()
    y_acc[...] = h_ref[...].astype(jnp.float32)
    by_token = jnp.concatenate([slot_row[...].astype(jnp.float32), gate_row[...], jnp.zeros((8 - 2 * slot_row.shape[0], tok), jnp.float32)], axis=0).T

    def combine(pattern):
        slots = (lax.broadcasted_iota(jnp.int32, (tok, rows), 1) + pattern * rows).astype(jnp.float32)
        z_blk = z_in[pattern]
        for choice in range(slot_row.shape[0]):
            chosen = (slots == by_token[:, choice:choice + 1]).astype(jnp.bfloat16)
            y_acc[...] = y_acc[...] + by_token[:, slot_row.shape[0] + choice:slot_row.shape[0] + choice + 1] * jnp.dot(chosen, z_blk, preferred_element_type=jnp.float32)

    backs = {}
    for turn, (first, second) in enumerate(rounds):
        for pattern in (first, second):
            if pattern:
                sends[pattern].wait_recv()
        for half in range(2):
            if turn == 0:
                loads[half * 3].wait()
                loads[half * 3 + 1].wait()

        x_blk = jnp.concatenate([recv[first], recv[second]], axis=0)

        def half_step(half, carry):
            for col in range(0, ffn, tile):
                gate_pre = jnp.dot(x_blk, w_gate[half, :, col:col + tile], preferred_element_type=jnp.float32)
                up_pre = jnp.dot(x_blk, w_up[half, :, col:col + tile], preferred_element_type=jnp.float32)
                act[half, :, col:col + tile] = (jax.nn.silu(gate_pre) * up_pre).astype(jnp.bfloat16)
            return carry

        lax.fori_loop(0, 2, half_step, 0)
        if turn == 0:
            for half in range(2):
                loads[half * 3 + 2].wait()

        def out_step(col, carry):
            at = pl.multiple_of(col * tile, tile)
            z_blk = jnp.dot(act[0], w_down[0, :, pl.ds(at, tile)], preferred_element_type=jnp.float32)
            z_blk = z_blk + jnp.dot(act[1], w_down[1, :, pl.ds(at, tile)], preferred_element_type=jnp.float32)
            z_blk = z_blk.astype(jnp.bfloat16)
            z_out[first, :, pl.ds(at, tile)] = z_blk[:rows]
            z_out[second, :, pl.ds(at, tile)] = z_blk[rows:]
            return carry

        lax.fori_loop(0, hid // tile, out_step, 0)
        for pattern in (first, second):
            if pattern:
                backs[pattern] = pltpu.make_async_remote_copy(
                    src_ref=z_out.at[pattern], dst_ref=z_in.at[pattern], send_sem=back_sem.at[pattern], recv_sem=home_sem.at[pattern],
                    device_id=peer(pattern), device_id_type=MESH_ID)
                backs[pattern].start()
    z_in[0] = z_out[0]
    combine(0)
    for pattern in order:
        backs[pattern].wait_recv()
        combine(pattern)
    result = pltpu.make_async_copy(y_acc, y_ref, own_sem.at[0])
    result.start()
    for pattern in order:
        sends[pattern].wait_send()
        backs[pattern].wait_send()
    result.wait()


def expert_layer(h_loc, slot_idx, gates, n_chips, own_weights, other_weights):
    tok, hid = h_loc.shape
    rows = slot_idx.shape[1] * tok // n_chips
    ffn = own_weights[0].shape[2]
    order = (1, 4, 6, 5, 7, 2, 3)
    rounds = ((0, 1), (4, 6), (5, 7), (2, 3))
    weights = []
    for own, other in zip(own_weights, other_weights):
        weights += [own, other]
    any_spec = pl.BlockSpec(memory_space=pl.ANY)
    vmem = pl.BlockSpec(memory_space=pltpu.VMEM)
    flops = 2 * 3 * n_chips * rows * hid * 2 * ffn
    return pl.pallas_call(
        functools.partial(expert_kernel, n_chips, order, rounds),
        out_shape=jax.ShapeDtypeStruct((tok, hid), jnp.float32),
        in_specs=[vmem] * 3 + [any_spec] * 6,
        out_specs=any_spec,
        scratch_shapes=[
            pltpu.VMEM((n_chips, rows, hid), jnp.bfloat16),
            pltpu.VMEM((n_chips, rows, hid), jnp.bfloat16),
            pltpu.VMEM((2, hid, ffn), jnp.bfloat16),
            pltpu.VMEM((2, hid, ffn), jnp.bfloat16),
            pltpu.VMEM((2, ffn, hid), jnp.bfloat16),
            pltpu.VMEM((2, 2 * rows, ffn), jnp.bfloat16),
            pltpu.VMEM((n_chips, rows, hid), jnp.bfloat16),
            pltpu.VMEM((n_chips, rows, hid), jnp.bfloat16),
            pltpu.VMEM((tok, hid), jnp.float32),
            pltpu.SemaphoreType.DMA((2, 3)),
            pltpu.SemaphoreType.DMA((1,)),
            pltpu.SemaphoreType.DMA((n_chips,)),
            pltpu.SemaphoreType.DMA((n_chips,)),
            pltpu.SemaphoreType.DMA((n_chips,)),
            pltpu.SemaphoreType.DMA((n_chips,)),
        ],
        compiler_params=pltpu.CompilerParams(collective_id=1, has_side_effects=True, vmem_limit_bytes=58 * 1024 * 1024),
        cost_estimate=pl.CostEstimate(flops=flops, bytes_accessed=32 * 1024 * 1024, transcendentals=n_chips * rows * 2 * ffn),
        name="expert_layer",
    )(h_loc, slot_idx.T, gates.T, *weights)


def solution(mesh):
    n_cp = mesh.shape["cp"]
    n_tp = mesh.shape["tp"]
    row_spec = P(("dp", "cp", "tp"), None)
    head_spec = P(None, "tp", None)
    expert_spec = P(("cp", "tp"), None, None)

    def device_step(x_loc, w_q, w_k, w_v, w_o, ids_loc, gates_loc, w_gate, w_up, w_down):
        tok_dev, hid_dim = x_loc.shape
        top_k = ids_loc.shape[1]
        heads = w_q.shape[1]
        head_dim = w_q.shape[2]
        local_exp = w_gate.shape[0]
        n_experts = local_exp * n_cp * n_tp // 2
        capacity = top_k * tok_dev // n_experts
        chip = lax.axis_index("cp") * 2 + lax.axis_index("tp") // 2

        choice_hot = (ids_loc[:, :, None] == jnp.arange(n_experts)[None, None, :])
        token_hot = jnp.sum(choice_hot.astype(jnp.bfloat16), axis=1)
        earlier = (lax.broadcasted_iota(jnp.int32, (tok_dev, tok_dev), 0) > lax.broadcasted_iota(jnp.int32, (tok_dev, tok_dev), 1)).astype(jnp.bfloat16)
        rank_in = jnp.dot(earlier, token_hot, preferred_element_type=jnp.float32).astype(jnp.int32)
        place = rank_in + (jnp.arange(n_experts, dtype=jnp.int32) ^ chip)[None, :] * capacity
        dest_idx = jnp.sum(jnp.where(choice_hot, place[:, None, :], 0), axis=2)

        w_qkv_t = [one.transpose(1, 2, 0).reshape(-1, hid_dim) for one in (w_q, w_k, w_v)]
        h_loc, *other_weights = attention(x_loc, *w_qkv_t, w_o.reshape(heads * head_dim, hid_dim), (w_gate, w_up, w_down), n_cp, n_tp, head_dim)
        return expert_layer(h_loc, dest_idx, gates_loc, n_experts, (w_gate, w_up, w_down), other_weights).astype(jnp.bfloat16)

    return jax.shard_map(device_step, mesh=mesh, in_specs=(row_spec, head_spec, head_spec, head_spec, P("tp", None, None), row_spec, row_spec, expert_spec, expert_spec, expert_spec), out_specs=row_spec, check_vma=False)
```
